256 devices in a mesh: blk: 64 (over x_lo, y, z), mp: 4 (over x_hi, core).
Axes of the slice: x: 4 (x_hi: 2, x_lo: 2; x = x_hi * 2 + x_lo), y: 4, z: 8, core: 2. Of those that a mesh axis runs over, the one named last changes fastest.
Arguments:
- tokens: bfloat16 [8192, 2048], P('blk', 'mp'), may hold values from -16 to 16
- grad_out: bfloat16 [8192, 2048], P('blk', 'mp'), may hold values from -0.29882812 to 0.29882812
- w_gate: bfloat16 [2048, 2560], P(None, 'mp'), may hold values from -0.125 to 0.125
- w_lin: bfloat16 [2048, 2560], P(None, 'mp'), may hold values from -0.125 to 0.125
- w_out_t: bfloat16 [2048, 2560], P(None, 'mp'), may hold values from -0.125 to 0.125
- code: float32 [64, 5], P('blk'), may hold values from 0.5 to 2
- decode: float32 [64], P('blk'), may hold values from 0.05 to 0.2
- stragglers: int32 [4], replicated, may hold values from 0 to 63, as said below
Outputs:
- grads: float32 [2048, 3, 2560], P('blk', None, 'mp')
The draws below stay inside these ranges and needn't reach their ends.
Inputs may be any that keep to these rules, and one draw needn't show every extreme that they name: `stragglers`: 4 distinct worker indices; worker 0 and worker 64 - 1 are always among them.
All inputs are finite; a program needn't handle non-finite values.
Results may differ from the reference program's by a relative error of at most 0.0042.
Values may be sent and summed in bfloat16 or wider, within the bound.
A program may use at most 128 MiB of HBM per device.

```python
import math
from functools import partial
import jax
import jax.numpy as jnp
from jax import lax

D = 2048
FF = 2560
S1 = 5
NSTRAG = 4
R = 128
TOKENS = 8192
N_BLK = 64


def draw_stragglers(key, part):
    order = jax.random.permutation(key, jnp.arange(N_BLK - 2, dtype=jnp.int32)) + 1
    ends = jnp.array([0, N_BLK - 1], dtype=jnp.int32)
    return jnp.concatenate([ends, order[:NSTRAG - 2]]).astype(jnp.int32)


def spiked(drawn, key, source, target, parts, factor):
    owner, partner = [(jnp.arange(drawn.shape[dim]) // (drawn.shape[dim] // parts)).reshape([-1 if axis == dim else 1 for axis in range(drawn.ndim)]) for dim in (source, target)]
    chosen = jax.random.permutation(key, parts)[partner]
    strong = (owner == chosen) | (owner == (partner + parts // 2) % parts)
    return jnp.where(strong, factor * drawn, drawn)


def level_of(key, dims, cuts, low, high):
    factor_of, own = 1.0, jax.random.fold_in(key, 6)
    for dim, shards_of in cuts:
        heights = jnp.exp(jax.random.uniform(jax.random.fold_in(own, dim), (shards_of,), jnp.float32, low / len(cuts), high / len(cuts)))
        factor_of = factor_of * jnp.repeat(heights, dims[dim] // shards_of).reshape([-1 if axis == dim else 1 for axis in range(len(dims))])
    return factor_of


def scatter_about(key, shape, width, reach, split=(), held_as=jnp.bfloat16):
    result = width * jax.random.normal(key, shape, jnp.float32)
    if split:
        result = result * level_of(key, shape, split, -0.22, 0.18)
    return jnp.clip(result, -reach, reach).astype(held_as)


def bell_draw_with(own_key, shape, deviation, limit, split, heavy, held_as=jnp.bfloat16):
    result = deviation * jax.random.normal(own_key, shape, jnp.float32)
    if split:
        result = result * level_of(own_key, shape, split, -0.22, 0.18)
    return jnp.clip(spiked(result, jax.random.fold_in(own_key, 3), *heavy), -limit, limit).astype(held_as)


def setup_inputs(seed: int = 0) -> dict:
    key_of = jax.random.split(jax.random.key(seed), 9)
    tokens = bell_draw_with(key_of[0], (TOKENS, D), 1.0, 16.0, ((0, 64), (1, 4)), (0, 1, 64, 4.0))
    grad_out = scatter_about(key_of[1], (TOKENS, D), 0.05, 0.29882812, ((0, 64), (1, 4)))
    w_gate = scatter_about(key_of[2], (D, FF), D ** -0.5, 0.125, ((1, 4),))
    w_lin = scatter_about(key_of[3], (D, FF), D ** -0.5, 0.125, ((1, 4),))
    w_out_t = scatter_about(key_of[4], (D, FF), FF ** -0.5, 0.125, ((1, 4),))
    code = jnp.clip(jnp.exp(math.log(2.0) - 1.3862944 * jax.random.uniform(key_of[5], (N_BLK, S1), jnp.float32) ** level_of(key_of[5], (N_BLK, S1), ((0, 64),), -0.2, 0.2)), 0.5, 2.0)
    decode = jnp.clip(jnp.exp(math.log(0.2) - 1.3862944 * jax.random.uniform(key_of[6], (N_BLK,), jnp.float32) ** level_of(key_of[6], (N_BLK,), ((0, 64),), -0.2, 0.2)), 0.05, 0.2)
    stragglers = draw_stragglers(jax.random.fold_in(key_of[8], 71), 0)
    return {"tokens": tokens, "grad_out": grad_out, "w_gate": w_gate, "w_lin": w_lin, "w_out_t": w_out_t, "code": code, "decode": decode, "stragglers": stragglers}


def local_grads(inputs, cotangent, w_gate, w_lin, w_out_t):
    gate_pre = jnp.dot(inputs, w_gate, preferred_element_type=jnp.float32)
    linear = jnp.dot(inputs, w_lin, preferred_element_type=jnp.float32)
    activated, pullback = jax.vjp(partial(jax.nn.gelu, approximate=True), gate_pre)
    hidden = (activated * linear).astype(jnp.bfloat16)
    hidden_grad = jnp.dot(cotangent, w_out_t, preferred_element_type=jnp.float32)
    d_gate = pullback(hidden_grad * linear)[0].astype(jnp.bfloat16)
    d_lin = (hidden_grad * activated).astype(jnp.bfloat16)
    return (jnp.concatenate([d_gate, d_lin], axis=1), hidden)

def reference(tokens, grad_out, w_gate, w_lin, w_out_t, code, decode, stragglers):
    worker_ids = jnp.arange(N_BLK, dtype=jnp.int32)
    is_alive = jnp.all(worker_ids[:, None] != stragglers[None, :], axis=1)
    own_decode = jnp.where(is_alive, decode, jnp.float32(0.0)).astype(jnp.float32)
    slot_ids = jnp.arange(S1, dtype=jnp.int32)
    owners = ((worker_ids[:, None] - slot_ids[None, :]) % N_BLK).astype(jnp.int32)
    slot_grid = jnp.broadcast_to(slot_ids[None, :], owners.shape)
    partition_weight = lax.optimization_barrier(jnp.sum(own_decode[owners] * code[owners, slot_grid], axis=1)).astype(jnp.float32)
    inputs = tokens.reshape(N_BLK, R, D)
    cotangents = grad_out.reshape(N_BLK, R, D)

    def accumulate(accum, items):
        inputs_p, cotangent_p, weight_p = items
        right_side, hidden = local_grads(inputs_p, cotangent_p, w_gate, w_lin, w_out_t)
        product = jnp.concatenate([jnp.dot(inputs_p.T, right_side, preferred_element_type=jnp.float32), jnp.dot(cotangent_p.T, hidden, preferred_element_type=jnp.float32)], axis=1)
        return (accum + weight_p * product, None)
    start_value = jnp.zeros((D, 3 * FF), jnp.float32)
    accum = lax.scan(accumulate, start_value, (inputs, cotangents, partition_weight))[0]
    return accum.reshape(D, 3, FF)
```

```python
import functools

import jax
import jax.numpy as jnp
from jax import lax
from jax.experimental import pallas as pl
from jax.experimental.pallas import tpu as pltpu
from jax.sharding import PartitionSpec as P

MESH = pl.DeviceIdType.MESH
BF16 = jnp.bfloat16
F32 = jnp.float32

NX, NY, NZ = 4, 4, 8
SIZE = {"y": NY, "z": NZ}
ROWS = 128
WIDTH = 512
HID = 640
OWN = 32
WLANES = 256

STREAMS = (
    ("z", "y", 0, 256, 1),
    ("z", "y", 256, 256, -1),
    ("z", "y", 512, 256, 1),
    ("z", "y", 768, 128, -1),
    ("y", "z", 896, 256, 1),
    ("y", "z", 1152, 256, -1),
    ("y", "z", 1408, 256, 1),
    ("y", "z", 1664, 256, -1),
)
SPLIT = 896


def steps_of(n, sigma):
    half = n // 2
    steps = []
    for t in range(1, half + 1):
        step = [(sigma, half + 1 - t, t - 1, t - 2 if t > 1 else None)]
        if t < half:
            step.append((-sigma, half - t, half + t - 1, half + t - 2 if t > 1 else None))
        steps.append(step)
    return steps


def last_slots(n):
    return (n // 2 - 1, n - 2)


def gelu_parts(u):
    c = 0.7978845608028654
    t = jnp.tanh(c * (u + 0.044715 * (u * u * u)))
    half = 0.5 * (1.0 + t)
    act = u * half
    slope = half + 0.5 * u * (1.0 - t * t) * (c * (1.0 + 3.0 * 0.044715 * (u * u)))
    return act, slope


def kernel(
    tok, gout, w_gate, w_lin, w_out, code, decode, strag,
    out,
    gath, wg, wl, wo, acc_g, acc_l, acc_h, dmat, xt, yt, prod, vec, wrecv, wpair, *rest,
):
    n_streams = len(STREAMS)
    snd1, rcv1 = rest[:n_streams], rest[n_streams : 2 * n_streams]
    snd2, rcv2 = rest[2 * n_streams : 3 * n_streams], rest[3 * n_streams : 4 * n_streams]
    mid = rest[4 * n_streams : 5 * n_streams]
    (loc_sem, gs_sem, gr_sem, ds_sem, dr_sem, ws_sem, wr_sem, s1, r1, s2, r2) = rest[5 * n_streams :]

    b = lax.axis_index("blk")
    m = lax.axis_index("mp")
    x_lo, yz = lax.div(b, NY * NZ), lax.rem(b, NY * NZ)
    y, z = lax.div(yz, NZ), lax.rem(yz, NZ)
    x_hi, core = lax.div(m, 2), lax.rem(m, 2)
    x = 2 * x_hi + x_lo
    me = {"y": y, "z": z}

    def device(px, py, pz, pc):
        return (lax.rem(px, 2) * (NY * NZ) + py * NZ + pz, lax.div(px, 2) * 2 + pc)

    def x_shift(d):
        return lax.rem(x + d + NX, NX)

    def ring_device(axis, d):
        q = lax.rem(me[axis] + d + SIZE[axis], SIZE[axis])
        return device(x, q, z, core) if axis == "y" else device(x, y, q, core)

    right, left = device(x_shift(1), y, z, core), device(x_shift(-1), y, z, core)
    sibling = device(x, y, z, 1 - core)
    pair = (lax.rem(b + NY * NZ, 2 * NY * NZ), m)

    mine = pl.ds(pl.multiple_of(x_lo * ROWS, ROWS), ROWS)
    load_x = pltpu.make_async_copy(tok, gath.at[m, 0, mine, :], loc_sem.at[0])
    load_y = pltpu.make_async_copy(gout, gath.at[m, 1, mine, :], loc_sem.at[1])
    load_x.start()
    load_y.start()
    loads_w = [
        pltpu.make_async_copy(src, dst, loc_sem.at[2 + i])
        for i, (src, dst) in enumerate(((w_gate, wg), (w_lin, wl), (w_out, wo)))
    ]
    for load in loads_w:
        load.start()

    barrier = pltpu.get_barrier_semaphore()
    partners = [right, left, sibling]
    partners += [ring_device(axis, d) for axis in ("y", "z") for d in (1, -1)]
    partners += [(lax.rem(b + d + 64, 64), m) for d in (1, 2, 3, 4, -1, -2, -3, -4)]
    for partner in partners:
        pl.semaphore_signal(barrier, inc=1, device_id=partner, device_id_type=MESH)

    alive = (strag[0] != b) & (strag[1] != b) & (strag[2] != b) & (strag[3] != b)
    own_decode = jnp.where(alive, decode[0], 0.0)
    row_id = lax.broadcasted_iota(jnp.int32, (8, WLANES), 0)
    coeffs = jnp.zeros((8, WLANES), F32)
    for j in range(5):
        coeffs = jnp.where(row_id == j, own_decode * code[0, j], coeffs)
    vec[...] = coeffs
    pl.semaphore_wait(barrier, len(partners))

    def remote(src, dst, ss, rs, to):
        return pltpu.make_async_remote_copy(
            src_ref=src, dst_ref=dst, send_sem=ss, recv_sem=rs, device_id=to, device_id_type=MESH
        )

    pending = []

    def go(src, dst, ss, rs, to):
        copy = remote(src, dst, ss, rs, to)
        copy.start()
        pending.append(copy)
        return copy

    def slot(px, pc, kind):
        rows = pl.ds(pl.multiple_of(lax.rem(px, 2) * ROWS, ROWS), ROWS)
        return gath.at[lax.div(px, 2) * 2 + pc, kind, rows, :]

    own_slot = [slot(x, core, k) for k in (0, 1)]
    load_x.wait()
    from_left = [None, None]
    from_right = [None, None]
    from_left[0] = go(own_slot[0], own_slot[0], gs_sem.at[0], gr_sem.at[0], right)
    load_y.wait()
    from_right[1] = go(own_slot[1], own_slot[1], gs_sem.at[3], gr_sem.at[3], left)
    from_left[1] = go(own_slot[1], own_slot[1], gs_sem.at[1], gr_sem.at[1], right)
    from_right[0] = go(own_slot[0], own_slot[0], gs_sem.at[2], gr_sem.at[2], left)
    sib = {}

    def to_sibling(rel, kind):
        src = slot(x_shift(rel), core, kind)
        idx = (rel % 4) * 2 + kind
        sib[rel, kind] = go(src, src, ds_sem.at[idx], dr_sem.at[idx], sibling)

    to_sibling(0, 0)
    to_sibling(0, 1)
    wcopies = [
        go(vec, wrecv.at[j - 1], ws_sem.at[j - 1], wr_sem.at[j - 1], (lax.rem(b + j, 64), m)) for j in (1, 2, 3, 4)
    ]
    from_left[0].wait_recv()
    left_x = slot(x_shift(-1), core, 0)
    far_x = go(left_x, left_x, gs_sem.at[4], gr_sem.at[4], right)
    to_sibling(-1, 0)
    from_right[1].wait_recv()
    right_y = slot(x_shift(1), core, 1)
    far_y = go(right_y, right_y, gs_sem.at[5], gr_sem.at[5], left)
    to_sibling(1, 1)
    for copy in wcopies:
        copy.wait_recv()
    total = vec[0:1, :]
    for j in (1, 2, 3, 4):
        total = total + wrecv[j - 1, j : j + 1, :]
    wpair[x_lo] = jnp.broadcast_to(total, (8, WLANES))
    wswap = go(wpair.at[x_lo], wpair.at[x_lo], ws_sem.at[4], wr_sem.at[4], pair)
    from_left[1].wait_recv()
    to_sibling(-1, 1)
    from_right[0].wait_recv()
    to_sibling(1, 0)
    for load in loads_w:
        load.wait()
    for rel in (0, -1, 1):
        for kind in (0, 1):
            sib[rel, kind].wait_recv()

    def forward(mm, first):
        ks = pl.ds(pl.multiple_of(mm * WIDTH, WIDTH), WIDTH)
        for kind, w, acc in ((0, wg, acc_g), (0, wl, acc_l), (1, wo, acc_h)):
            part = jnp.dot(gath[mm, kind], w[ks, :], preferred_element_type=F32)
            acc[...] = part if first else acc[...] + part

    forward(2 * x_hi, True)
    forward(2 * x_hi + 1, False)
    far_x.wait_recv()
    to_sibling(2, 0)
    far_y.wait_recv()
    to_sibling(2, 1)
    forward(2 * (1 - x_hi) + core, False)
    sib[2, 0].wait_recv()
    sib[2, 1].wait_recv()
    forward(2 * (1 - x_hi) + 1 - core, False)
    for i in range(2):
        xt[pl.ds(i * WIDTH, WIDTH), :] = gath[2 * x_lo + i, 0].T
        yt[pl.ds(i * WIDTH, WIDTH), :] = gath[2 * x_lo + i, 1].T

    def elementwise(i, carry):
        rows = pl.ds(pl.multiple_of(i * 16, 16), 16)
        act, slope = gelu_parts(acc_g[rows, :])
        lin, dh = acc_l[rows, :], acc_h[rows, :]
        dmat[rows, 0:HID] = (dh * lin * slope).astype(BF16)
        dmat[rows, HID : 2 * HID] = (dh * act).astype(BF16)
        dmat[rows, 2 * HID :] = (act * lin).astype(BF16)
        return carry

    lax.fori_loop(0, 2 * ROWS // 16, elementwise, 0)
    wswap.wait_recv()
    weight = [wpair[i, 0:1, :] for i in (0, 1)]

    def products(yd, lower, upper):
        rows = pl.ds(pl.multiple_of(yd * (NZ * OWN), NZ * OWN), NZ * OWN)
        col = lower
        while col < upper:
            stop = min(upper, col + 256)
            if col < 2 * HID:
                stop = min(stop, 2 * HID)
            lhs = xt if col < 2 * HID else yt
            width = stop - col
            value = None
            for i in (0, 1):
                tokens = slice(i * ROWS, (i + 1) * ROWS)
                part = jnp.dot(lhs[rows, tokens], dmat[tokens, col:stop], preferred_element_type=F32)
                part = weight[i][:, :width] * part
                value = part if value is None else value + part
            prod[yd, :, :, col:stop] = value.reshape(NZ, OWN, width)
            col = stop

    def local1(s, d):
        axis, _, col, width, _ = STREAMS[s]
        cols = slice(col, col + width)
        return prod[:, d, :, cols] if axis == "z" else prod[d, :, :, cols]

    def run(s):
        axis1, axis2, col, width, sigma = STREAMS[s]
        for phase, axis, snd, rcv, ss, rs in ((1, axis1, snd1[s], rcv1[s], s1, r1), (2, axis2, snd2[s], rcv2[s], s2, r2)):
            n = SIZE[axis]
            local = functools.partial(local1, s) if phase == 1 else lambda d: mid[s][d]
            base = s * 8
            flying = {}
            for step in steps_of(n, sigma):
                for direction, distance, index, before in step:
                    yield (s, phase, "send", direction, distance)
                    dest = lax.rem(me[axis] + direction * distance + n, n)
                    value = local(dest)
                    if before is not None:
                        flying[before].wait_recv()
                        value = value + rcv[before].astype(F32)
                    snd[index] = value.astype(BF16)
                    flying[index] = go(
                        snd.at[index], rcv.at[index], ss.at[base + index], rs.at[base + index],
                        ring_device(axis, direction),
                    )
            yield (s, phase, "sum")
            value = local(me[axis])
            for index in last_slots(n):
                flying[index].wait_recv()
                value = value + rcv[index].astype(F32)
            if phase == 1:
                mid[s][...] = value
            else:
                out[:, col : col + width] = value

    runs = [run(s) for s in range(n_streams)]
    heads = [next(r) for r in runs]

    def advance(s, until):
        while heads[s] is not None and not until(heads[s]):
            heads[s] = next(runs[s], None)

    y_first = [s for s in range(n_streams) if STREAMS[s][0] == "y"]
    z_first = [s for s in range(n_streams) if STREAMS[s][0] == "z"]
    far = lax.rem(y + 2, NY)
    products(far, SPLIT, 3 * HID)
    for s in y_first[:2]:
        advance(s, lambda h: h[4] != 2)
    for d in range(NY):
        products(jnp.int32(d), 0, SPLIT)
    for s in z_first:
        advance(s, lambda h: h[4] != 4)
    products(lax.rem(y + 1, NY), SPLIT, 3 * HID)
    products(lax.rem(y + 3, NY), SPLIT, 3 * HID)
    for s in y_first[:2]:
        advance(s, lambda h: h[2] == "sum" or h[4] == 1 and h[3] == STREAMS[s][4])
    for s in z_first:
        advance(s, lambda h: h[2] == "sum" or h[4] <= 3 and h[3] == STREAMS[s][4])
    products(y, SPLIT, 3 * HID)
    order = []
    for _ in range(24):
        order += y_first + z_first
    for s in order:
        if heads[s] is not None:
            heads[s] = next(runs[s], None)
    assert all(h is None for h in heads)
    for copy in pending:
        copy.wait_send()


def shards(tokens, grad_out, w_gate, w_lin, w_out_t, code, decode, stragglers):
    n = len(STREAMS)
    scratch = [
        pltpu.VMEM((4, 2, 2 * ROWS, WIDTH), BF16),
        pltpu.VMEM((4 * WIDTH, HID), BF16),
        pltpu.VMEM((4 * WIDTH, HID), BF16),
        pltpu.VMEM((4 * WIDTH, HID), BF16),
        pltpu.VMEM((2 * ROWS, HID), F32),
        pltpu.VMEM((2 * ROWS, HID), F32),
        pltpu.VMEM((2 * ROWS, HID), F32),
        pltpu.VMEM((2 * ROWS, 3 * HID), BF16),
        pltpu.VMEM((2 * WIDTH, 2 * ROWS), BF16),
        pltpu.VMEM((2 * WIDTH, 2 * ROWS), BF16),
        pltpu.VMEM((NY, NZ, OWN, 3 * HID), F32),
        pltpu.VMEM((8, WLANES), F32),
        pltpu.VMEM((4, 8, WLANES), F32),
        pltpu.VMEM((2, 8, WLANES), F32),
    ]
    first = [pltpu.VMEM((SIZE[a] - 1, SIZE[c], OWN, w), BF16) for a, c, _, w, _ in STREAMS]
    second = [pltpu.VMEM((SIZE[c] - 1, OWN, w), BF16) for a, c, _, w, _ in STREAMS]
    scratch += first + first + second + second
    scratch += [pltpu.VMEM((SIZE[c], OWN, w), F32) for a, c, _, w, _ in STREAMS]
    dma = pltpu.SemaphoreType.DMA
    scratch += [dma((5,)), dma((6,)), dma((6,)), dma((8,)), dma((8,)), dma((5,)), dma((5,))]
    scratch += [dma((8 * n,)), dma((8 * n,)), dma((8 * n,)), dma((8 * n,))]
    hbm, smem = pl.BlockSpec(memory_space=pl.ANY), pl.BlockSpec(memory_space=pltpu.SMEM)
    result = pl.pallas_call(
        kernel,
        out_shape=jax.ShapeDtypeStruct((OWN, 3 * HID), F32),
        in_specs=[hbm] * 5 + [smem] * 3,
        out_specs=pl.BlockSpec(memory_space=pltpu.VMEM),
        scratch_shapes=scratch,
        compiler_params=pltpu.CompilerParams(
            collective_id=0, has_side_effects=True, vmem_limit_bytes=60 * 1024 * 1024
        ),
    )(tokens, grad_out, w_gate, w_lin, w_out_t, code, decode, stragglers)
    return result.reshape(OWN, 3, HID)


def solution(mesh):
    in_specs = (
        P("blk", "mp"),
        P("blk", "mp"),
        P(None, "mp"),
        P(None, "mp"),
        P(None, "mp"),
        P("blk", None),
        P("blk"),
        P(),
    )
    out_specs = P("blk", None, "mp")
    return jax.shard_map(shards, mesh=mesh, in_specs=in_specs, out_specs=out_specs, check_vma=False)
```

```python
import functools

import jax
import jax.numpy as jnp
from jax import lax
from jax.experimental import pallas as pl
from jax.experimental.pallas import tpu as pltpu
from jax.sharding import PartitionSpec as P

MESH = pl.DeviceIdType.MESH
BF16 = jnp.bfloat16
F32 = jnp.float32

NX, NY, NZ = 4, 4, 8
SIZE = {"y": NY, "z": NZ}
ROWS = 128
WIDTH = 512
HID = 640
OWN = 32
LANES = 128

STREAMS = (
    ("y", "z", 1408, 128, 1),
    ("y", "z", 640, 128, -1),
    ("y", "z", 896, 128, -1),
    ("y", "z", 1664, 128, -1),
    ("y", "z", 1152, 128, -1),
    ("z", "y", 1024, 128, 1),
    ("z", "y", 256, 256, -1),
    ("y", "z", 128, 128, 1),
    ("y", "z", 512, 128, 1),
    ("z", "y", 0, 128, 1),
    ("z", "y", 1792, 128, 1),
    ("z", "y", 1280, 128, 1),
    ("z", "y", 768, 128, -1),
    ("y", "z", 1536, 128, 1),
)
ORDER = (
    7, 7, 1, 1, 9, 9, 6, 6, 6, 7, 1, 0, 0, 9, 12, 12, 11, 11, 2, 2, 2, 13, 13, 9, 13, 7, 3, 1, 3, 5,
    5, 5, 12, 11, 0, 3, 8, 6, 8, 6, 8, 4, 4, 9, 4, 11, 10, 10, 12, 9, 2, 10, 0, 5, 5, 12, 11, 6, 1, 13,
    1, 1, 6, 11, 9, 10, 3, 7, 7, 7, 12, 9, 10, 5, 5, 12, 11, 8, 6, 1, 1, 4, 11, 10, 7, 7, 12, 2, 2, 0,
    0, 2, 9, 9, 10, 0, 9, 5, 3, 13, 13, 3, 13, 3, 11, 11, 11, 4, 8, 8, 4, 8, 6, 1, 10, 7, 6, 4, 0, 7,
    1, 9, 6, 12, 12, 12, 2, 2, 5, 5, 13, 5, 0, 11, 3, 3, 13, 8, 4, 8, 1, 6, 9, 10, 10, 10, 7, 12, 4, 2,
    0, 5, 2, 13, 0, 11, 3, 3, 13, 8, 4, 8, 1, 6, 10, 7, 12, 4, 2, 0, 5, 13, 3, 8, 4, 10, 2, 0, 13, 3,
    8, 4,
)
BLOCKS = ((0, 256), (256, 512), (512, 640))


def steps_of(n, sigma):
    half = n // 2
    steps = []
    for t in range(1, half + 1):
        step = [(sigma, half + 1 - t, t - 1, t - 2 if t > 1 else None)]
        if t < half:
            step.append((-sigma, half - t, half + t - 1, half + t - 2 if t > 1 else None))
        steps.append(step)
    return steps


def last_slots(n):
    return (n // 2 - 1, n - 2)


def gelu_parts(u):
    c = 0.7978845608028654
    t = jnp.tanh(c * (u + 0.044715 * (u * u * u)))
    half = 0.5 * (1.0 + t)
    act = u * half
    slope = half + 0.5 * u * (1.0 - t * t) * (c * (1.0 + 3.0 * 0.044715 * (u * u)))
    return act, slope


def kernel(
    tok, gout, w_gate, w_lin, w_out, code, decode, strag,
    out,
    code_s, decode_s, strag_s, stage,
    gath, wg, wl, wo, acc_g, acc_l, acc_h, dmat, xt, yt, prod, tab, ytab, *rest,
):
    n_streams = len(STREAMS)
    snd1, rcv1 = rest[:n_streams], rest[n_streams : 2 * n_streams]
    snd2, rcv2 = rest[2 * n_streams : 3 * n_streams], rest[3 * n_streams : 4 * n_streams]
    mid = rest[4 * n_streams : 5 * n_streams]
    (loc_sem, gs_sem, gr_sem, ds_sem, dr_sem, ws_sem, wr_sem, out_sem, s1, r1, s2, r2) = rest[5 * n_streams :]

    b = lax.axis_index("blk")
    m = lax.axis_index("mp")
    x_lo, yz = lax.div(b, NY * NZ), lax.rem(b, NY * NZ)
    y, z = lax.div(yz, NZ), lax.rem(yz, NZ)
    x_hi, core = lax.div(m, 2), lax.rem(m, 2)
    x = 2 * x_hi + x_lo
    me = {"y": y, "z": z}

    def device(px, py, pz, pc):
        return (lax.rem(px, 2) * (NY * NZ) + py * NZ + pz, lax.div(px, 2) * 2 + pc)

    def x_shift(d):
        return lax.rem(x + d + NX, NX)

    def ring_device(axis, d):
        q = lax.rem(me[axis] + d + SIZE[axis], SIZE[axis])
        return device(x, q, z, core) if axis == "y" else device(x, y, q, core)

    right, left = device(x_shift(1), y, z, core), device(x_shift(-1), y, z, core)
    sibling = device(x, y, z, 1 - core)
    pair = (lax.rem(b + NY * NZ, 2 * NY * NZ), m)

    barrier = pltpu.get_barrier_semaphore()
    partners = [right, left, sibling]
    partners += [ring_device(axis, d) for axis in ("y", "z") for d in (1, -1)]
    partners += [ring_device("z", -2)]
    for partner in partners:
        pl.semaphore_signal(barrier, inc=1, device_id=partner, device_id_type=MESH)

    smalls = [
        pltpu.make_async_copy(source, dest, loc_sem.at[5 + i])
        for i, (source, dest) in enumerate(((code, code_s), (decode, decode_s), (strag, strag_s)))
    ]
    for load in smalls:
        load.start()
    mine = pl.ds(pl.multiple_of(x_lo * ROWS, ROWS), ROWS)
    load_x = pltpu.make_async_copy(tok, gath.at[m, 0, mine, :], loc_sem.at[0])
    load_y = pltpu.make_async_copy(gout, gath.at[m, 1, mine, :], loc_sem.at[1])
    load_x.start()
    load_y.start()
    loads_w = [
        pltpu.make_async_copy(source, dest, loc_sem.at[2 + i])
        for i, (source, dest) in enumerate(((w_gate, wg), (w_lin, wl), (w_out, wo)))
    ]
    for load in loads_w:
        load.start()

    for load in smalls:
        load.wait()
    alive = (strag_s[0] != b) & (strag_s[1] != b) & (strag_s[2] != b) & (strag_s[3] != b)
    own_decode = jnp.where(alive, decode_s[0], 0.0)
    row_id = lax.broadcasted_iota(jnp.int32, (8, LANES), 0)
    coeffs = jnp.zeros((8, LANES), F32)
    for j in range(5):
        coeffs = jnp.where(row_id == j, own_decode * code_s[0, j], coeffs)
    tab[0, x_lo] = coeffs
    pl.semaphore_wait(barrier, len(partners))

    def remote(src, dst, ss, rs, to):
        return pltpu.make_async_remote_copy(
            src_ref=src, dst_ref=dst, send_sem=ss, recv_sem=rs, device_id=to, device_id_type=MESH
        )

    pending = []

    def go(src, dst, ss, rs, to):
        copy = remote(src, dst, ss, rs, to)
        copy.start()
        pending.append(copy)
        return copy

    def slot(px, pc, kind):
        rows = pl.ds(pl.multiple_of(lax.rem(px, 2) * ROWS, ROWS), ROWS)
        return gath.at[lax.div(px, 2) * 2 + pc, kind, rows, :]

    own_slot = [slot(x, core, k) for k in (0, 1)]
    swap = go(tab.at[0, x_lo], tab.at[0, x_lo], ws_sem.at[0], wr_sem.at[0], pair)
    load_x.wait()
    from_left = [None, None]
    from_right = [None, None]
    from_left[0] = go(own_slot[0], own_slot[0], gs_sem.at[0], gr_sem.at[0], right)
    load_y.wait()
    from_right[1] = go(own_slot[1], own_slot[1], gs_sem.at[3], gr_sem.at[3], left)
    from_left[1] = go(own_slot[1], own_slot[1], gs_sem.at[1], gr_sem.at[1], right)
    from_right[0] = go(own_slot[0], own_slot[0], gs_sem.at[2], gr_sem.at[2], left)
    sib = {}

    def to_sibling(rel, kind):
        src = slot(x_shift(rel), core, kind)
        idx = (rel % 4) * 2 + kind
        sib[rel, kind] = go(src, src, ds_sem.at[idx], dr_sem.at[idx], sibling)

    to_sibling(0, 0)
    to_sibling(0, 1)
    swap.wait_recv()
    near = [go(tab.at[0], tab.at[d], ws_sem.at[d], wr_sem.at[d], ring_device("z", d)) for d in (1, 2)]
    from_left[0].wait_recv()
    left_x = slot(x_shift(-1), core, 0)
    far_x = go(left_x, left_x, gs_sem.at[4], gr_sem.at[4], right)
    to_sibling(-1, 0)
    from_right[1].wait_recv()
    right_y = slot(x_shift(1), core, 1)
    far_y = go(right_y, right_y, gs_sem.at[5], gr_sem.at[5], left)
    to_sibling(1, 1)
    for copy in near:
        copy.wait_recv()
    farther = go(tab.at[pl.ds(1, 2)], tab.at[pl.ds(3, 2)], ws_sem.at[3], wr_sem.at[3], ring_device("z", 2))
    from_left[1].wait_recv()
    to_sibling(-1, 1)
    from_right[0].wait_recv()
    to_sibling(1, 0)
    farther.wait_recv()
    from_y = go(tab.at[pl.ds(1, 4)], ytab, ws_sem.at[4], wr_sem.at[4], ring_device("y", 1))
    for load in loads_w:
        load.wait()
    for rel in (0, -1, 1):
        for kind in (0, 1):
            sib[rel, kind].wait_recv()

    def forward(mm, first, lower=0, upper=HID):
        ks = pl.ds(pl.multiple_of(mm * WIDTH, WIDTH), WIDTH)
        cols = slice(lower, upper)
        for kind, w, acc in ((0, wg, acc_g), (0, wl, acc_l), (1, wo, acc_h)):
            part = jnp.dot(gath[mm, kind], w[ks, cols], preferred_element_type=F32)
            acc[:, cols] = part if first else acc[:, cols] + part

    forward(2 * x_hi, True)
    forward(2 * x_hi + 1, False)
    far_x.wait_recv()
    to_sibling(2, 0)
    far_y.wait_recv()
    to_sibling(2, 1)
    forward(2 * (1 - x_hi) + core, False)
    sib[2, 0].wait_recv()
    sib[2, 1].wait_recv()
    for i in range(2):
        xt[pl.ds(i * WIDTH, WIDTH), :] = gath[2 * x_lo + i, 0].T
        yt[pl.ds(i * WIDTH, WIDTH), :] = gath[2 * x_lo + i, 1].T
    from_y.wait_recv()
    weight = []
    for a in (0, 1):
        total = tab[0, a, 0:1, :]
        other = jnp.where(y == 0, 1 - a, a)
        for j in (1, 2, 3, 4):
            total = total + jnp.where(z >= j, tab[j, a, j : j + 1, :], ytab[j - 1, other, j : j + 1, :])
        weight.append(jnp.concatenate([total, total], axis=1))

    finished = set()

    def finish(block):
        lower, upper = BLOCKS[block]
        forward(2 * (1 - x_hi) + 1 - core, False, lower, upper)

        def elementwise(i, carry):
            rows = pl.ds(pl.multiple_of(i * 32, 32), 32)
            act, slope = gelu_parts(acc_g[rows, lower:upper])
            lin, dh = acc_l[rows, lower:upper], acc_h[rows, lower:upper]
            dmat[rows, lower:upper] = (dh * lin * slope).astype(BF16)
            dmat[rows, HID + lower : HID + upper] = (dh * act).astype(BF16)
            dmat[rows, 2 * HID + lower : 2 * HID + upper] = (act * lin).astype(BF16)
            return carry

        lax.fori_loop(0, 2 * ROWS // 32, elementwise, 0)

    def products(s):
        col, width = STREAMS[s][2:4]
        for block, (lower, upper) in enumerate(BLOCKS):
            if block not in finished and col % HID < upper and col % HID + width > lower:
                finished.add(block)
                finish(block)
        lhs = xt if col < 2 * HID else yt
        for yd in range(NY):
            rows = slice(yd * NZ * OWN, (yd + 1) * NZ * OWN)
            value = None
            for i in (0, 1):
                tokens = slice(i * ROWS, (i + 1) * ROWS)
                part = jnp.dot(lhs[rows, tokens], dmat[tokens, col : col + width], preferred_element_type=F32)
                part = weight[i][:, :width] * part
                value = part if value is None else value + part
            prod[yd, :, :, col : col + width] = value.reshape(NZ, OWN, width)

    def local1(s, d):
        axis, _, col, width, _ = STREAMS[s]
        cols = slice(col, col + width)
        return prod[:, d, :, cols] if axis == "z" else prod[d, :, :, cols]

    def run(s):
        axis1, axis2, col, width, sigma = STREAMS[s]
        yield
        products(s)
        for phase, axis, snd, rcv, ss, rs in ((1, axis1, snd1[s], rcv1[s], s1, r1), (2, axis2, snd2[s], rcv2[s], s2, r2)):
            n = SIZE[axis]
            local = functools.partial(local1, s) if phase == 1 else lambda d: mid[s][d]
            base = s * 8
            flying = {}
            for step in steps_of(n, sigma):
                for direction, distance, index, before in step:
                    yield
                    dest = lax.rem(me[axis] + direction * distance + n, n)
                    value = local(dest)
                    if before is not None:
                        flying[before].wait_recv()
                        value = value + rcv[before].astype(F32)
                    snd[index] = value.astype(BF16)
                    flying[index] = go(
                        snd.at[index], rcv.at[index], ss.at[base + index], rs.at[base + index],
                        ring_device(axis, direction),
                    )
            yield
            value = local(me[axis])
            for index in last_slots(n):
                flying[index].wait_recv()
                value = value + rcv[index].astype(F32)
            if phase == 1:
                mid[s][...] = value
            else:
                kind, cols = col // HID, pl.ds(col % HID, width)
                stage[kind, :, cols] = value
                written = pltpu.make_async_copy(stage.at[kind, :, cols], out.at[kind, :, cols], out_sem.at[s])
                written.start()
                writes.append(written)

    runs = [run(s) for s in range(n_streams)]
    writes = []
    for r in runs:
        next(r)
    for s in ORDER:
        next(runs[s], None)
    assert len(writes) == n_streams
    for written in writes:
        written.wait()
    for copy in pending:
        copy.wait_send()


def shards(tokens, grad_out, w_gate, w_lin, w_out_t, code, decode, stragglers):
    n = len(STREAMS)
    scratch = [
        pltpu.SMEM((1, 5), F32),
        pltpu.SMEM((1,), F32),
        pltpu.SMEM((4,), jnp.int32),
        pltpu.VMEM((3, OWN, HID), F32),
        pltpu.VMEM((4, 2, 2 * ROWS, WIDTH), BF16),
        pltpu.VMEM((4 * WIDTH, HID), BF16),
        pltpu.VMEM((4 * WIDTH, HID), BF16),
        pltpu.VMEM((4 * WIDTH, HID), BF16),
        pltpu.VMEM((2 * ROWS, HID), F32),
        pltpu.VMEM((2 * ROWS, HID), F32),
        pltpu.VMEM((2 * ROWS, HID), F32),
        pltpu.VMEM((2 * ROWS, 3 * HID), BF16),
        pltpu.VMEM((2 * WIDTH, 2 * ROWS), BF16),
        pltpu.VMEM((2 * WIDTH, 2 * ROWS), BF16),
        pltpu.VMEM((NY, NZ, OWN, 3 * HID), F32),
        pltpu.VMEM((5, 2, 8, LANES), F32),
        pltpu.VMEM((4, 2, 8, LANES), F32),
    ]
    first = [pltpu.VMEM((SIZE[a] - 1, SIZE[c], OWN, w), BF16) for a, c, _, w, _ in STREAMS]
    second = [pltpu.VMEM((SIZE[c] - 1, OWN, w), BF16) for a, c, _, w, _ in STREAMS]
    scratch += first + first + second + second
    scratch += [pltpu.VMEM((SIZE[c], OWN, w), F32) for a, c, _, w, _ in STREAMS]
    dma = pltpu.SemaphoreType.DMA
    scratch += [dma((8,)), dma((6,)), dma((6,)), dma((8,)), dma((8,)), dma((5,)), dma((5,)), dma((n,))]
    scratch += [dma((8 * n,)), dma((8 * n,)), dma((8 * n,)), dma((8 * n,))]
    hbm = pl.BlockSpec(memory_space=pl.ANY)
    result = pl.pallas_call(
        kernel,
        out_shape=jax.ShapeDtypeStruct((3, OWN, HID), F32),
        in_specs=[hbm] * 8,
        out_specs=hbm,
        scratch_shapes=scratch,
        compiler_params=pltpu.CompilerParams(
            collective_id=0, has_side_effects=True, vmem_limit_bytes=60 * 1024 * 1024
        ),
    )(tokens, grad_out, w_gate, w_lin, w_out_t, code, decode, stragglers)
    return jnp.swapaxes(result, 0, 1)


def solution(mesh):
    in_specs = (
        P("blk", "mp"),
        P("blk", "mp"),
        P(None, "mp"),
        P(None, "mp"),
        P(None, "mp"),
        P("blk", None),
        P("blk"),
        P(),
    )
    out_specs = P("blk", None, "mp")
    return jax.shard_map(shards, mesh=mesh, in_specs=in_specs, out_specs=out_specs, check_vma=False)
```

```python
import functools

import jax
import jax.numpy as jnp
from jax import lax
from jax.experimental import pallas as pl
from jax.experimental.pallas import tpu as pltpu
from jax.sharding import PartitionSpec as P

MESH = pl.DeviceIdType.MESH
BF16 = jnp.bfloat16
F32 = jnp.float32

NX, NY, NZ = 4, 4, 8
SIZE = {"y": NY, "z": NZ}
ROWS = 128
WIDTH = 512
HID = 640
OWN = 32
LANES = 128

STREAMS = (
    ("y", "z", 640, 256, -1, 0),
    ("z", "y", 896, 256, 1, 0),
    ("z", "y", 1792, 128, -1, 0),
    ("y", "z", 0, 256, 1, 0),
    ("y", "z", 1664, 128, -1, 0),
    ("y", "z", 1152, 128, -1, 0),
    ("z", "y", 256, 256, -1, 0),
    ("y", "z", 1536, 128, 1, 0),
    ("z", "y", 1280, 256, 1, 0),
    ("y", "z", 512, 128, 1, 0),
)
ORDER = (
    0, 0, 3, 3, 8, 8, 6, 6, 6, 1, 1, 0, 1, 8, 3, 4, 4, 7, 7, 4, 7, 9, 9, 9, 2, 2, 2, 5, 5, 5,
    8, 0, 3, 6, 6, 1, 1, 8, 4, 2, 2, 8, 7, 6, 6, 1, 1, 9, 5, 8, 2, 2, 8, 6, 0, 0, 0, 3, 3, 3,
    1, 4, 4, 4, 7, 7, 7, 5, 5, 5, 2, 9, 9, 9, 8, 8, 8, 3, 6, 6, 6, 0, 0, 3, 1, 4, 1, 1, 4, 7,
    5, 7, 5, 9, 8, 2, 2, 2, 9, 3, 6, 0, 0, 3, 4, 1, 4, 7, 5, 5, 7, 9, 8, 2, 9, 3, 6, 0, 4, 1,
    7, 5, 9, 2, 3, 0, 4, 7, 5, 9,
)
BLOCKS = ((0, 256), (256, 512), (512, 640))


def steps_of(n, sigma):
    half = n // 2
    steps = []
    for t in range(1, half + 1):
        index = t - 1 if t < half else n - 3
        steps.append((sigma, half + 1 - t, index, t - 2 if t > 1 else None))
        if t < half:
            index = half + t - 2 if t < half - 1 else n - 2
            steps.append((-sigma, half - t, index, half + t - 3 if t > 1 else None))
    return steps


def sems_of(n, direct):
    return 1 if direct else n - 2


def counts():
    first, total = [], 0
    for a, c, _, _, _, direct in STREAMS:
        first.append((total, total + sems_of(SIZE[a], 0)))
        total = first[-1][1] + sems_of(SIZE[c], direct)
    return first, total


def gelu_parts(u):
    c = 0.7978845608028654
    t = jnp.tanh(c * (u + 0.044715 * (u * u * u)))
    half = 0.5 * (1.0 + t)
    act = u * half
    slope = half + 0.5 * u * (1.0 - t * t) * (c * (1.0 + 3.0 * 0.044715 * (u * u)))
    return act, slope


def kernel(
    tok, gout, w_gate, w_lin, w_out, code, decode, strag,
    out,
    code_s, decode_s, strag_s, stage,
    gath, wg, wl, wo, acc_g, acc_l, acc_h, dmat, xt, yt, prod, tab, ytab, *rest,
):
    n_streams = len(STREAMS)
    snd1, rcv1 = rest[:n_streams], rest[n_streams : 2 * n_streams]
    snd2, rcv2 = rest[2 * n_streams : 3 * n_streams], rest[3 * n_streams : 4 * n_streams]
    mid = rest[4 * n_streams : 5 * n_streams]
    (loc_sem, gs_sem, gr_sem, ds_sem, dr_sem, ws_sem, wr_sem, out_sem, s_sem, r_sem) = rest[5 * n_streams :]

    b = lax.axis_index("blk")
    m = lax.axis_index("mp")
    x_lo, yz = lax.div(b, NY * NZ), lax.rem(b, NY * NZ)
    y, z = lax.div(yz, NZ), lax.rem(yz, NZ)
    x_hi, core = lax.div(m, 2), lax.rem(m, 2)
    x = 2 * x_hi + x_lo
    me = {"y": y, "z": z}

    def device(px, py, pz, pc):
        return (lax.rem(px, 2) * (NY * NZ) + py * NZ + pz, lax.div(px, 2) * 2 + pc)

    def x_shift(d):
        return lax.rem(x + d + NX, NX)

    def ring_device(axis, d):
        q = lax.rem(me[axis] + d + SIZE[axis], SIZE[axis])
        return device(x, q, z, core) if axis == "y" else device(x, y, q, core)

    right, left = device(x_shift(1), y, z, core), device(x_shift(-1), y, z, core)
    sibling = device(x, y, z, 1 - core)
    pair = (lax.rem(b + NY * NZ, 2 * NY * NZ), m)

    barrier = pltpu.get_barrier_semaphore()
    partners = [right, left, sibling]
    partners += [ring_device(axis, d) for axis in ("y", "z") for d in (1, -1)]
    partners += [ring_device("z", -2)]
    for partner in partners:
        pl.semaphore_signal(barrier, inc=1, device_id=partner, device_id_type=MESH)

    smalls = [
        pltpu.make_async_copy(source, dest, loc_sem.at[5 + i])
        for i, (source, dest) in enumerate(((code, code_s), (decode, decode_s), (strag, strag_s)))
    ]
    for load in smalls:
        load.start()
    mine = pl.ds(pl.multiple_of(x_lo * ROWS, ROWS), ROWS)
    load_x = pltpu.make_async_copy(tok, gath.at[m, 0, mine, :], loc_sem.at[0])
    load_y = pltpu.make_async_copy(gout, gath.at[m, 1, mine, :], loc_sem.at[1])
    load_x.start()
    load_y.start()
    loads_w = [
        pltpu.make_async_copy(source, dest, loc_sem.at[2 + i])
        for i, (source, dest) in enumerate(((w_gate, wg), (w_lin, wl), (w_out, wo)))
    ]
    for load in loads_w:
        load.start()

    for load in smalls:
        load.wait()
    alive = (strag_s[0] != b) & (strag_s[1] != b) & (strag_s[2] != b) & (strag_s[3] != b)
    own_decode = jnp.where(alive, decode_s[0], 0.0)
    row_id = lax.broadcasted_iota(jnp.int32, (8, LANES), 0)
    coeffs = jnp.zeros((8, LANES), F32)
    for j in range(5):
        coeffs = jnp.where(row_id == j, own_decode * code_s[0, j], coeffs)
    tab[0, x_lo] = coeffs
    pl.semaphore_wait(barrier, len(partners))

    def remote(src, dst, ss, rs, to):
        return pltpu.make_async_remote_copy(
            src_ref=src, dst_ref=dst, send_sem=ss, recv_sem=rs, device_id=to, device_id_type=MESH
        )

    pending = []

    def go(src, dst, ss, rs, to):
        copy = remote(src, dst, ss, rs, to)
        copy.start()
        pending.append(copy)
        return copy

    def slot(px, pc, kind):
        rows = pl.ds(pl.multiple_of(lax.rem(px, 2) * ROWS, ROWS), ROWS)
        return gath.at[lax.div(px, 2) * 2 + pc, kind, rows, :]

    own_slot = [slot(x, core, k) for k in (0, 1)]
    swap = go(tab.at[0, x_lo], tab.at[0, x_lo], ws_sem.at[0], wr_sem.at[0], pair)
    load_x.wait()
    from_left = [None, None]
    from_right = [None, None]
    from_left[0] = go(own_slot[0], own_slot[0], gs_sem.at[0], gr_sem.at[0], right)
    load_y.wait()
    from_right[1] = go(own_slot[1], own_slot[1], gs_sem.at[3], gr_sem.at[3], left)
    from_left[1] = go(own_slot[1], own_slot[1], gs_sem.at[1], gr_sem.at[1], right)
    from_right[0] = go(own_slot[0], own_slot[0], gs_sem.at[2], gr_sem.at[2], left)
    sib = {}

    def to_sibling(rel, kind):
        src = slot(x_shift(rel), core, kind)
        idx = (rel % 4) * 2 + kind
        sib[rel, kind] = go(src, src, ds_sem.at[idx], dr_sem.at[idx], sibling)

    to_sibling(0, 0)
    to_sibling(0, 1)
    swap.wait_recv()
    near = [go(tab.at[0], tab.at[d], ws_sem.at[d], wr_sem.at[d], ring_device("z", d)) for d in (1, 2)]
    from_left[0].wait_recv()
    left_x = slot(x_shift(-1), core, 0)
    far_x = go(left_x, left_x, gs_sem.at[4], gr_sem.at[4], right)
    to_sibling(-1, 0)
    from_right[1].wait_recv()
    right_y = slot(x_shift(1), core, 1)
    far_y = go(right_y, right_y, gs_sem.at[5], gr_sem.at[5], left)
    to_sibling(1, 1)
    for copy in near:
        copy.wait_recv()
    farther = go(tab.at[pl.ds(1, 2)], tab.at[pl.ds(3, 2)], ws_sem.at[3], wr_sem.at[3], ring_device("z", 2))
    for load in loads_w:
        load.wait()
    from_left[1].wait_recv()
    to_sibling(-1, 1)
    from_right[0].wait_recv()
    to_sibling(1, 0)

    def forward(mm, first, lower=0, upper=HID):
        ks = pl.ds(pl.multiple_of(mm * WIDTH, WIDTH), WIDTH)
        cols = slice(lower, upper)
        for kind, w, acc in ((0, wg, acc_g), (0, wl, acc_l), (1, wo, acc_h)):
            part = jnp.dot(gath[mm, kind], w[ks, cols], preferred_element_type=F32)
            acc[:, cols] = part if first else acc[:, cols] + part

    def transpose(a):
        tokens = pl.ds(pl.multiple_of(a * ROWS, ROWS), ROWS)
        for i in range(2):
            xt[pl.ds(i * WIDTH, WIDTH), tokens] = gath[2 * x_lo + i, 0, tokens, :].T
            yt[pl.ds(i * WIDTH, WIDTH), tokens] = gath[2 * x_lo + i, 1, tokens, :].T

    forward(2 * x_hi + core, True)
    for rel in (0, -1, 1):
        for kind in (0, 1):
            sib[rel, kind].wait_recv()
    farther.wait_recv()
    from_y = go(tab.at[pl.ds(1, 4)], ytab, ws_sem.at[4], wr_sem.at[4], ring_device("y", 1))
    forward(2 * x_hi + 1 - core, False)
    far_x.wait_recv()
    to_sibling(2, 0)
    far_y.wait_recv()
    to_sibling(2, 1)
    forward(2 * (1 - x_hi) + core, False)
    transpose(1 - x_lo)
    sib[2, 0].wait_recv()
    sib[2, 1].wait_recv()
    transpose(x_lo)
    from_y.wait_recv()
    weight = []
    for a in (0, 1):
        total = tab[0, a, 0:1, :]
        other = jnp.where(y == 0, 1 - a, a)
        for j in (1, 2, 3, 4):
            total = total + jnp.where(z >= j, tab[j, a, j : j + 1, :], ytab[j - 1, other, j : j + 1, :])
        weight.append(jnp.concatenate([total, total], axis=1))

    finished = set()

    def finish(block):
        lower, upper = BLOCKS[block]
        forward(2 * (1 - x_hi) + 1 - core, False, lower, upper)

        def elementwise(i, carry):
            rows = pl.ds(pl.multiple_of(i * 32, 32), 32)
            act, slope = gelu_parts(acc_g[rows, lower:upper])
            lin, dh = acc_l[rows, lower:upper], acc_h[rows, lower:upper]
            dmat[rows, lower:upper] = (dh * lin * slope).astype(BF16)
            dmat[rows, HID + lower : HID + upper] = (dh * act).astype(BF16)
            dmat[rows, 2 * HID + lower : 2 * HID + upper] = (act * lin).astype(BF16)
            return carry

        lax.fori_loop(0, 2 * ROWS // 32, elementwise, 0)

    def products(s):
        col, width = STREAMS[s][2:4]
        for block, (lower, upper) in enumerate(BLOCKS):
            if block not in finished and col % HID < upper and col % HID + width > lower:
                finished.add(block)
                finish(block)
        lhs = xt if col < 2 * HID else yt
        for yd in range(NY):
            rows = slice(yd * NZ * OWN, (yd + 1) * NZ * OWN)
            value = None
            for i in (0, 1):
                tokens = slice(i * ROWS, (i + 1) * ROWS)
                part = jnp.dot(lhs[rows, tokens], dmat[tokens, col : col + width], preferred_element_type=F32)
                part = weight[i][:, :width] * part
                value = part if value is None else value + part
            prod[yd, :, :, col : col + width] = value.reshape(NZ, OWN, width)

    def local1(s, d):
        axis, _, col, width = STREAMS[s][:4]
        cols = slice(col, col + width)
        return prod[:, d, :, cols] if axis == "z" else prod[d, :, :, cols]

    def run(s):
        axis1, axis2, col, width, sigma, direct2 = STREAMS[s]
        yield
        products(s)
        for phase, axis, snd, rcv in ((0, axis1, snd1[s], rcv1[s]), (1, axis2, snd2[s], rcv2[s])):
            n = SIZE[axis]
            local = functools.partial(local1, s) if phase == 0 else lambda d: mid[s][d]
            ss, base = s_sem.at[2 * s + phase], first_sem[s][phase]
            sent.append((snd, ss))
            if phase and direct2:
                for k in range(n - 1, 0, -1):
                    yield
                    snd[k - 1] = local(lax.rem(me[axis] + k, n)).astype(BF16)
                    to = ring_device(axis, k if 2 * k <= n else k - n)
                    remote(snd.at[k - 1], rcv.at[k - 1], ss, r_sem.at[base], to).start()
                yield
                remote(snd, rcv, ss, r_sem.at[base], sibling).wait_recv()
                arrived = range(n - 1)
            else:
                for direction, distance, index, before in steps_of(n, sigma):
                    yield
                    value = local(lax.rem(me[axis] + direction * distance + n, n))
                    to = ring_device(axis, direction)
                    if before is not None:
                        remote(snd.at[before], rcv.at[before], ss, r_sem.at[base + before], to).wait_recv()
                        value = value + rcv[before].astype(F32)
                    snd[index] = value.astype(BF16)
                    remote(snd.at[index], rcv.at[index], ss, r_sem.at[base + min(index, n - 3)], to).start()
                yield
                last = pl.ds(n - 3, 2)
                remote(snd.at[last], rcv.at[last], ss, r_sem.at[base + n - 3], sibling).wait_recv()
                arrived = (n - 3, n - 2)
            value = local(me[axis])
            for index in arrived:
                value = value + rcv[index].astype(F32)
            if phase == 0:
                mid[s][...] = value
            else:
                kind, cols = col // HID, pl.ds(col % HID, width)
                stage[kind, :, cols] = value
                written = pltpu.make_async_copy(stage.at[kind, :, cols], out.at[kind, :, cols], out_sem.at[s])
                written.start()
                writes.append(written)

    first_sem, _ = counts()
    sent = []
    runs = [run(s) for s in range(n_streams)]
    writes = []
    for r in runs:
        next(r)
    for s in ORDER:
        next(runs[s], None)
    assert len(writes) == n_streams
    for written in writes:
        written.wait()
    for snd, ss in sent:
        remote(snd, snd, ss, r_sem.at[0], sibling).wait_send()
    for copy in pending:
        copy.wait_send()


def shards(tokens, grad_out, w_gate, w_lin, w_out_t, code, decode, stragglers):
    n = len(STREAMS)
    scratch = [
        pltpu.SMEM((1, 5), F32),
        pltpu.SMEM((1,), F32),
        pltpu.SMEM((4,), jnp.int32),
        pltpu.VMEM((3, OWN, HID), F32),
        pltpu.VMEM((4, 2, 2 * ROWS, WIDTH), BF16),
        pltpu.VMEM((4 * WIDTH, HID), BF16),
        pltpu.VMEM((4 * WIDTH, HID), BF16),
        pltpu.VMEM((4 * WIDTH, HID), BF16),
        pltpu.VMEM((2 * ROWS, HID), F32),
        pltpu.VMEM((2 * ROWS, HID), F32),
        pltpu.VMEM((2 * ROWS, HID), F32),
        pltpu.VMEM((2 * ROWS, 3 * HID), BF16),
        pltpu.VMEM((2 * WIDTH, 2 * ROWS), BF16),
        pltpu.VMEM((2 * WIDTH, 2 * ROWS), BF16),
        pltpu.VMEM((NY, NZ, OWN, 3 * HID), F32),
        pltpu.VMEM((5, 2, 8, LANES), F32),
        pltpu.VMEM((4, 2, 8, LANES), F32),
    ]
    first = [pltpu.VMEM((SIZE[a] - 1, SIZE[c], OWN, w), BF16) for a, c, _, w, _, _ in STREAMS]
    second = [pltpu.VMEM((SIZE[c] - 1, OWN, w), BF16) for a, c, _, w, _, _ in STREAMS]
    scratch += first + first + second + second
    scratch += [pltpu.VMEM((SIZE[c], OWN, w), F32) for a, c, _, w, _, _ in STREAMS]
    dma = pltpu.SemaphoreType.DMA
    scratch += [dma((8,)), dma((6,)), dma((6,)), dma((8,)), dma((8,)), dma((5,)), dma((5,)), dma((n,))]
    scratch += [dma((2 * n,)), dma((counts()[1],))]
    hbm = pl.BlockSpec(memory_space=pl.ANY)
    result = pl.pallas_call(
        kernel,
        out_shape=jax.ShapeDtypeStruct((3, OWN, HID), F32),
        in_specs=[hbm] * 8,
        out_specs=hbm,
        scratch_shapes=scratch,
        compiler_params=pltpu.CompilerParams(
            collective_id=0, has_side_effects=True, vmem_limit_bytes=60 * 1024 * 1024
        ),
    )(tokens, grad_out, w_gate, w_lin, w_out_t, code, decode, stragglers)
    return jnp.swapaxes(result, 0, 1)


def solution(mesh):
    in_specs = (
        P("blk", "mp"),
        P("blk", "mp"),
        P(None, "mp"),
        P(None, "mp"),
        P(None, "mp"),
        P("blk", None),
        P("blk"),
        P(),
    )
    out_specs = P("blk", None, "mp")
    return jax.shard_map(shards, mesh=mesh, in_specs=in_specs, out_specs=out_specs, check_vma=False)
```

```python
import functools

import jax
import jax.numpy as jnp
from jax import lax
from jax.experimental import pallas as pl
from jax.experimental.pallas import tpu as pltpu
from jax.sharding import PartitionSpec as P

MESH = pl.DeviceIdType.MESH
BF16 = jnp.bfloat16
F32 = jnp.float32

NX, NY, NZ = 4, 4, 8
SIZE = {"y": NY, "z": NZ}
ROWS = 128
WIDTH = 512
HID = 640
OWN = 32
LANES = 128

STREAMS = (
    ("y", "z", 1280, 128, 1, 0),
    ("z", "y", 1152, 128, 1, 0),
    ("y", "z", 512, 128, 1, 0),
    ("y", "z", 256, 128, 1, 1),
    ("y", "z", 1536, 256, 1, 1),
    ("y", "z", 0, 256, -1, 0),
    ("y", "z", 384, 128, 1, 1),
    ("z", "y", 640, 256, 1, 0),
    ("z", "y", 1792, 128, -1, 0),
    ("z", "y", 896, 256, -1, 0),
    ("z", "y", 1408, 128, -1, 0),
)
ORDER = (
    2, 2, 2, 1, 1, 1, 8, 8, 8, 0, 0, 0, 10, 10, 10, 7, 7, 7, 5, 5, 5, 9, 1, 1, 9, 9, 6, 6, 6, 4,
    2, 8, 8, 4, 4, 3, 3, 3, 10, 10, 0, 7, 7, 1, 1, 5, 9, 9, 8, 8, 6, 10, 10, 2, 2, 2, 7, 7, 1, 9,
    9, 4, 8, 10, 3, 2, 2, 5, 5, 0, 0, 0, 5, 7, 1, 1, 1, 6, 6, 6, 6, 6, 9, 8, 8, 8, 2, 0, 10, 10,
    10, 2, 5, 5, 0, 4, 4, 4, 4, 4, 7, 7, 7, 8, 3, 3, 3, 3, 3, 1, 2, 6, 10, 0, 6, 6, 9, 9, 9, 5,
    5, 0, 7, 8, 4, 1, 10, 4, 4, 2, 3, 9, 3, 3, 0, 5, 6, 7, 4, 9, 0, 3, 5,
)
BLOCKS = ((0, 256), (256, 512), (512, 640))


def schedule(n, sigma, two_stage):
    half = n // 2
    if two_stage:
        messages = [
            (sigma, 2, 4, 0, None),
            (sigma, 2, 3, 1, None),
            (-sigma, 2, 3, 2, None),
            (-sigma, 2, 2, 3, None),
            (sigma, 2, 2, 4, 0),
            (sigma, 1, 1, 5, 1),
            (-sigma, 1, 1, 6, 2),
        ]
        return messages, 4
    messages = []
    for t in range(1, half + 1):
        index = t - 1 if t < half else n - 3
        messages.append((sigma, 1, half + 1 - t, index, t - 2 if t > 1 else None))
        if t < half:
            index = half + t - 2 if t < half - 1 else n - 2
            messages.append((-sigma, 1, half - t, index, half + t - 3 if t > 1 else None))
    return messages, 2


def counts():
    first, total = [], 0
    for a, c, _, _, sigma, two_stage in STREAMS:
        middle = total + SIZE[a] - schedule(SIZE[a], sigma, 0)[1]
        first.append((total, middle))
        total = middle + SIZE[c] - schedule(SIZE[c], sigma, two_stage)[1]
    return first, total


def gelu_parts(u):
    c = 0.7978845608028654
    t = jnp.tanh(c * (u + 0.044715 * (u * u * u)))
    half = 0.5 * (1.0 + t)
    act = u * half
    slope = half + 0.5 * u * (1.0 - t * t) * (c * (1.0 + 3.0 * 0.044715 * (u * u)))
    return act, slope


def kernel(
    tok, gout, w_gate, w_lin, w_out, code, decode, strag,
    out,
    code_s, decode_s, strag_s, stage,
    gath, wg, wl, wo, acc_g, acc_l, acc_h, dmat, xt, yt, prod, tab, ytab, *rest,
):
    n_streams = len(STREAMS)
    snd1, rcv1 = rest[:n_streams], rest[n_streams : 2 * n_streams]
    snd2, rcv2 = rest[2 * n_streams : 3 * n_streams], rest[3 * n_streams : 4 * n_streams]
    mid = rest[4 * n_streams : 5 * n_streams]
    (loc_sem, gs_sem, gr_sem, ds_sem, dr_sem, ws_sem, wr_sem, out_sem, s_sem, r_sem) = rest[5 * n_streams :]

    b = lax.axis_index("blk")
    m = lax.axis_index("mp")
    x_lo, yz = lax.div(b, NY * NZ), lax.rem(b, NY * NZ)
    y, z = lax.div(yz, NZ), lax.rem(yz, NZ)
    x_hi, core = lax.div(m, 2), lax.rem(m, 2)
    x = 2 * x_hi + x_lo
    me = {"y": y, "z": z}

    def device(px, py, pz, pc):
        return (lax.rem(px, 2) * (NY * NZ) + py * NZ + pz, lax.div(px, 2) * 2 + pc)

    def x_shift(d):
        return lax.rem(x + d + NX, NX)

    def ring_device(axis, d):
        q = lax.rem(me[axis] + d + SIZE[axis], SIZE[axis])
        return device(x, q, z, core) if axis == "y" else device(x, y, q, core)

    right, left = device(x_shift(1), y, z, core), device(x_shift(-1), y, z, core)
    sibling = device(x, y, z, 1 - core)
    pair = (lax.rem(b + NY * NZ, 2 * NY * NZ), m)

    barrier = pltpu.get_barrier_semaphore()
    partners = [right, left, sibling]
    partners += [ring_device(axis, d) for axis in ("y", "z") for d in (1, -1)]
    partners += [ring_device("z", d) for d in (2, -2)]
    for partner in partners:
        pl.semaphore_signal(barrier, inc=1, device_id=partner, device_id_type=MESH)

    smalls = [
        pltpu.make_async_copy(source, dest, loc_sem.at[5 + i])
        for i, (source, dest) in enumerate(((code, code_s), (decode, decode_s), (strag, strag_s)))
    ]
    for load in smalls:
        load.start()
    mine = pl.ds(pl.multiple_of(x_lo * ROWS, ROWS), ROWS)
    load_x = pltpu.make_async_copy(tok, gath.at[m, 0, mine, :], loc_sem.at[0])
    load_y = pltpu.make_async_copy(gout, gath.at[m, 1, mine, :], loc_sem.at[1])
    load_x.start()
    load_y.start()
    loads_w = [
        pltpu.make_async_copy(source, dest, loc_sem.at[2 + i])
        for i, (source, dest) in enumerate(((w_gate, wg), (w_lin, wl), (w_out, wo)))
    ]
    for load in loads_w:
        load.start()

    for load in smalls:
        load.wait()
    alive = (strag_s[0] != b) & (strag_s[1] != b) & (strag_s[2] != b) & (strag_s[3] != b)
    own_decode = jnp.where(alive, decode_s[0], 0.0)
    row_id = lax.broadcasted_iota(jnp.int32, (8, LANES), 0)
    coeffs = jnp.zeros((8, LANES), F32)
    for j in range(5):
        coeffs = jnp.where(row_id == j, own_decode * code_s[0, j], coeffs)
    tab[0, x_lo] = coeffs
    pl.semaphore_wait(barrier, len(partners))

    def remote(src, dst, ss, rs, to):
        return pltpu.make_async_remote_copy(
            src_ref=src, dst_ref=dst, send_sem=ss, recv_sem=rs, device_id=to, device_id_type=MESH
        )

    pending = []

    def go(src, dst, ss, rs, to):
        copy = remote(src, dst, ss, rs, to)
        copy.start()
        pending.append(copy)
        return copy

    def slot(px, pc, kind):
        rows = pl.ds(pl.multiple_of(lax.rem(px, 2) * ROWS, ROWS), ROWS)
        return gath.at[lax.div(px, 2) * 2 + pc, kind, rows, :]

    own_slot = [slot(x, core, k) for k in (0, 1)]
    swap = go(tab.at[0, x_lo], tab.at[0, x_lo], ws_sem.at[0], wr_sem.at[0], pair)
    load_x.wait()
    from_left = [None, None]
    from_right = [None, None]
    from_left[0] = go(own_slot[0], own_slot[0], gs_sem.at[0], gr_sem.at[0], right)
    load_y.wait()
    from_right[1] = go(own_slot[1], own_slot[1], gs_sem.at[3], gr_sem.at[3], left)
    from_left[1] = go(own_slot[1], own_slot[1], gs_sem.at[1], gr_sem.at[1], right)
    from_right[0] = go(own_slot[0], own_slot[0], gs_sem.at[2], gr_sem.at[2], left)
    sib = {}

    def to_sibling(rel, kind):
        src = slot(x_shift(rel), core, kind)
        idx = (rel % 4) * 2 + kind
        sib[rel, kind] = go(src, src, ds_sem.at[idx], dr_sem.at[idx], sibling)

    to_sibling(0, 0)
    to_sibling(0, 1)
    swap.wait_recv()
    near = [go(tab.at[0], tab.at[d], ws_sem.at[d], wr_sem.at[d], ring_device("z", d)) for d in (1, 2)]
    from_left[0].wait_recv()
    left_x = slot(x_shift(-1), core, 0)
    far_x = go(left_x, left_x, gs_sem.at[4], gr_sem.at[4], right)
    to_sibling(-1, 0)
    from_right[1].wait_recv()
    right_y = slot(x_shift(1), core, 1)
    far_y = go(right_y, right_y, gs_sem.at[5], gr_sem.at[5], left)
    to_sibling(1, 1)
    for copy in near:
        copy.wait_recv()
    farther = go(tab.at[pl.ds(1, 2)], tab.at[pl.ds(3, 2)], ws_sem.at[3], wr_sem.at[3], ring_device("z", 2))
    for load in loads_w:
        load.wait()
    from_left[1].wait_recv()
    to_sibling(-1, 1)
    from_right[0].wait_recv()
    to_sibling(1, 0)

    def forward(mm, first, lower=0, upper=HID):
        ks = pl.ds(pl.multiple_of(mm * WIDTH, WIDTH), WIDTH)
        cols = slice(lower, upper)
        for kind, w, acc in ((0, wg, acc_g), (0, wl, acc_l), (1, wo, acc_h)):
            part = jnp.dot(gath[mm, kind], w[ks, cols], preferred_element_type=F32)
            acc[:, cols] = part if first else acc[:, cols] + part

    def transpose(a):
        tokens = pl.ds(pl.multiple_of(a * ROWS, ROWS), ROWS)
        for i in range(2):
            xt[pl.ds(i * WIDTH, WIDTH), tokens] = gath[2 * x_lo + i, 0, tokens, :].T
            yt[pl.ds(i * WIDTH, WIDTH), tokens] = gath[2 * x_lo + i, 1, tokens, :].T

    forward(2 * x_hi + core, True)
    for rel in (0, -1, 1):
        for kind in (0, 1):
            sib[rel, kind].wait_recv()
    farther.wait_recv()
    from_y = go(tab.at[pl.ds(1, 4)], ytab, ws_sem.at[4], wr_sem.at[4], ring_device("y", 1))
    forward(2 * x_hi + 1 - core, False)
    far_x.wait_recv()
    to_sibling(2, 0)
    far_y.wait_recv()
    to_sibling(2, 1)
    forward(2 * (1 - x_hi) + core, False)
    transpose(1 - x_lo)
    sib[2, 0].wait_recv()
    sib[2, 1].wait_recv()
    transpose(x_lo)
    from_y.wait_recv()
    weight = []
    for a in (0, 1):
        total = tab[0, a, 0:1, :]
        other = jnp.where(y == 0, 1 - a, a)
        for j in (1, 2, 3, 4):
            total = total + jnp.where(z >= j, tab[j, a, j : j + 1, :], ytab[j - 1, other, j : j + 1, :])
        weight.append(jnp.concatenate([total, total], axis=1))

    finished = set()

    def finish(block):
        lower, upper = BLOCKS[block]
        forward(2 * (1 - x_hi) + 1 - core, False, lower, upper)

        def elementwise(i, carry):
            rows = pl.ds(pl.multiple_of(i * 32, 32), 32)
            act, slope = gelu_parts(acc_g[rows, lower:upper])
            lin, dh = acc_l[rows, lower:upper], acc_h[rows, lower:upper]
            dmat[rows, lower:upper] = (dh * lin * slope).astype(BF16)
            dmat[rows, HID + lower : HID + upper] = (dh * act).astype(BF16)
            dmat[rows, 2 * HID + lower : 2 * HID + upper] = (act * lin).astype(BF16)
            return carry

        lax.fori_loop(0, 2 * ROWS // 32, elementwise, 0)

    def products(s):
        col, width = STREAMS[s][2:4]
        for block, (lower, upper) in enumerate(BLOCKS):
            if block not in finished and col % HID < upper and col % HID + width > lower:
                finished.add(block)
                finish(block)
        lhs = xt if col < 2 * HID else yt
        for yd in range(NY):
            rows = slice(yd * NZ * OWN, (yd + 1) * NZ * OWN)
            value = None
            for i in (0, 1):
                tokens = slice(i * ROWS, (i + 1) * ROWS)
                part = jnp.dot(lhs[rows, tokens], dmat[tokens, col : col + width], preferred_element_type=F32)
                part = weight[i][:, :width] * part
                value = part if value is None else value + part
            prod[yd, :, :, col : col + width] = value.reshape(NZ, OWN, width)

    def local1(s, d):
        axis, _, col, width = STREAMS[s][:4]
        cols = slice(col, col + width)
        return prod[:, d, :, cols] if axis == "z" else prod[d, :, :, cols]

    def run(s):
        axis1, axis2, col, width, sigma, two_stage = STREAMS[s]
        yield
        products(s)
        for phase, axis, snd, rcv in ((0, axis1, snd1[s], rcv1[s]), (1, axis2, snd2[s], rcv2[s])):
            n = SIZE[axis]
            local = functools.partial(local1, s) if phase == 0 else lambda d: mid[s][d]
            ss, base = s_sem.at[2 * s + phase], first_sem[s][phase]
            sent.append((snd, ss))
            messages, finals = schedule(n, sigma, phase and two_stage)
            middle = n - 1 - finals
            for direction, hops, distance, index, before in messages:
                yield
                value = local(lax.rem(me[axis] + direction * distance + n, n))
                to = ring_device(axis, direction * hops)
                if before is not None:
                    remote(snd.at[before], rcv.at[before], ss, r_sem.at[base + before], to).wait_recv()
                    value = value + rcv[before].astype(F32)
                snd[index] = value.astype(BF16)
                remote(snd.at[index], rcv.at[index], ss, r_sem.at[base + min(index, middle)], to).start()
            yield
            last = pl.ds(middle, finals)
            remote(snd.at[last], rcv.at[last], ss, r_sem.at[base + middle], sibling).wait_recv()
            arrived = range(middle, n - 1)
            value = local(me[axis])
            for index in arrived:
                value = value + rcv[index].astype(F32)
            if phase == 0:
                mid[s][...] = value
            else:
                kind, cols = col // HID, pl.ds(col % HID, width)
                out[kind, :, cols] = value

    first_sem, _ = counts()
    sent = []
    runs = [run(s) for s in range(n_streams)]
    for r in runs:
        next(r)
    for s in ORDER:
        next(runs[s], None)
    for snd, ss in sent:
        remote(snd, snd, ss, r_sem.at[0], sibling).wait_send()
    for copy in pending:
        copy.wait_send()


def shards(tokens, grad_out, w_gate, w_lin, w_out_t, code, decode, stragglers):
    n = len(STREAMS)
    scratch = [
        pltpu.SMEM((1, 5), F32),
        pltpu.SMEM((1,), F32),
        pltpu.SMEM((4,), jnp.int32),
        pltpu.VMEM((3, OWN, HID), F32),
        pltpu.VMEM((4, 2, 2 * ROWS, WIDTH), BF16),
        pltpu.VMEM((4 * WIDTH, HID), BF16),
        pltpu.VMEM((4 * WIDTH, HID), BF16),
        pltpu.VMEM((4 * WIDTH, HID), BF16),
        pltpu.VMEM((2 * ROWS, HID), F32),
        pltpu.VMEM((2 * ROWS, HID), F32),
        pltpu.VMEM((2 * ROWS, HID), F32),
        pltpu.VMEM((2 * ROWS, 3 * HID), BF16),
        pltpu.VMEM((2 * WIDTH, 2 * ROWS), BF16),
        pltpu.VMEM((2 * WIDTH, 2 * ROWS), BF16),
        pltpu.VMEM((NY, NZ, OWN, 3 * HID), F32),
        pltpu.VMEM((5, 2, 8, LANES), F32),
        pltpu.VMEM((4, 2, 8, LANES), F32),
    ]
    first = [pltpu.VMEM((SIZE[a] - 1, SIZE[c], OWN, w), BF16) for a, c, _, w, _, _ in STREAMS]
    second = [pltpu.VMEM((SIZE[c] - 1, OWN, w), BF16) for a, c, _, w, _, _ in STREAMS]
    scratch += first + first + second + second
    scratch += [pltpu.VMEM((SIZE[c], OWN, w), F32) for a, c, _, w, _, _ in STREAMS]
    dma = pltpu.SemaphoreType.DMA
    scratch += [dma((8,)), dma((6,)), dma((6,)), dma((8,)), dma((8,)), dma((5,)), dma((5,)), dma((n,))]
    scratch += [dma((2 * n,)), dma((counts()[1],))]
    hbm = pl.BlockSpec(memory_space=pl.ANY)
    result = pl.pallas_call(
        kernel,
        out_shape=pltpu.VMEM((3, OWN, HID), F32),
        in_specs=[hbm] * 8,
        out_specs=pl.BlockSpec(memory_space=pltpu.VMEM),
        scratch_shapes=scratch,
        compiler_params=pltpu.CompilerParams(
            collective_id=0, has_side_effects=True, vmem_limit_bytes=60 * 1024 * 1024
        ),
    )(tokens, grad_out, w_gate, w_lin, w_out_t, code, decode, stragglers)
    return jnp.swapaxes(result, 0, 1)


def solution(mesh):
    in_specs = (
        P("blk", "mp"),
        P("blk", "mp"),
        P(None, "mp"),
        P(None, "mp"),
        P(None, "mp"),
        P("blk", None),
        P("blk"),
        P(),
    )
    out_specs = P("blk", None, "mp")
    return jax.shard_map(shards, mesh=mesh, in_specs=in_specs, out_specs=out_specs, check_vma=False)
```

```python
import functools

import jax
import jax.numpy as jnp
from jax import lax
from jax.experimental import pallas as pl
from jax.experimental.pallas import tpu as pltpu
from jax.sharding import PartitionSpec as P

MESH = pl.DeviceIdType.MESH
BF16 = jnp.bfloat16
F32 = jnp.float32

NX, NY, NZ = 4, 4, 8
SIZE = {"y": NY, "z": NZ}
ROWS = 128
WIDTH = 512
HID = 640
OWN = 32
LANES = 128

STREAMS = (
    ("y", "z", 1280, 128, -1, 1),
    ("y", "z", 0, 128, 1, 1),
    ("y", "z", 1408, 128, 1, 0),
    ("z", "y", 1536, 128, -1, 0),
    ("z", "y", 1664, 256, -1, 0),
    ("y", "z", 640, 128, -1, 1),
    ("z", "y", 768, 256, 1, 0),
    ("y", "z", 384, 256, -1, 1),
    ("y", "z", 1024, 256, 1, 1),
    ("z", "y", 128, 256, 1, 0),
)
ORDER = (
    2, 2, 2, 3, 3, 3, 9, 9, 9, 8, 8, 8, 4, 4, 4, 6, 6, 6, 0, 0, 0, 5, 5, 5, 7, 3, 3, 7, 1, 2,
    1, 7, 1, 9, 9, 4, 4, 8, 6, 6, 3, 3, 0, 9, 9, 5, 4, 4, 2, 2, 2, 6, 6, 7, 1, 3, 9, 0, 0, 0,
    0, 0, 4, 2, 2, 5, 5, 5, 5, 5, 6, 8, 8, 8, 8, 8, 3, 3, 3, 9, 9, 9, 1, 1, 7, 7, 7, 7, 0, 1,
    1, 7, 1, 0, 2, 0, 4, 4, 4, 2, 3, 5, 9, 6, 6, 6, 5, 5, 8, 4, 8, 3, 8, 7, 1, 7, 9, 7, 6, 1,
    1, 2, 0, 4, 5, 8, 6, 7, 1, 2,
)
BLOCKS = ((0, 128), (128, 384), (384, 640))


def schedule(n, sigma, two_stage):
    half = n // 2
    if two_stage and n == 4:
        return [(sigma, 2, 2, 0, None), (1, 1, 1, 1, None), (-1, 1, 1, 2, None)], 3
    if two_stage:
        messages = [
            (sigma, 2, 4, 0, None),
            (sigma, 2, 3, 1, None),
            (-sigma, 2, 3, 2, None),
            (-sigma, 2, 2, 3, None),
            (sigma, 2, 2, 4, 0),
            (sigma, 1, 1, 5, 1),
            (-sigma, 1, 1, 6, 2),
        ]
        return messages, 4
    messages = []
    for t in range(1, half + 1):
        index = t - 1 if t < half else n - 3
        messages.append((sigma, 1, half + 1 - t, index, t - 2 if t > 1 else None))
        if t < half:
            index = half + t - 2 if t < half - 1 else n - 2
            messages.append((-sigma, 1, half - t, index, half + t - 3 if t > 1 else None))
    return messages, 2


def counts():
    first, total = [], 0
    for a, c, _, _, sigma, two_stage in STREAMS:
        middle = total + SIZE[a] - schedule(SIZE[a], sigma, 0)[1]
        first.append((total, middle))
        total = middle + SIZE[c] - schedule(SIZE[c], sigma, two_stage)[1]
    return first, total


def gelu_parts(u):
    c = 0.7978845608028654
    t = jnp.tanh(c * (u + 0.044715 * (u * u * u)))
    half = 0.5 * (1.0 + t)
    act = u * half
    slope = half + 0.5 * u * (1.0 - t * t) * (c * (1.0 + 3.0 * 0.044715 * (u * u)))
    return act, slope


def kernel(
    tok, gout, w_gate, w_lin, w_out, code, decode, strag,
    out,
    code_s, decode_s, strag_s,
    gath, wts, acc_g, acc_l, acc_h, dmat, xt, yt, prod, tab, ytab, *rest,
):
    n_streams = len(STREAMS)
    snd1, rcv1 = rest[:n_streams], rest[n_streams : 2 * n_streams]
    snd2, rcv2 = rest[2 * n_streams : 3 * n_streams], rest[3 * n_streams : 4 * n_streams]
    mid = rest[4 * n_streams : 5 * n_streams]
    (loc_sem, gs_sem, gr_sem, dr_sem, ws_sem, wr_sem, s_sem, r_sem) = rest[5 * n_streams :]

    b = lax.axis_index("blk")
    m = lax.axis_index("mp")
    x_lo, yz = lax.div(b, NY * NZ), lax.rem(b, NY * NZ)
    y, z = lax.div(yz, NZ), lax.rem(yz, NZ)
    x_hi, core = lax.div(m, 2), lax.rem(m, 2)
    x = 2 * x_hi + x_lo
    me = {"y": y, "z": z}

    def device(px, py, pz, pc):
        return (lax.rem(px, 2) * (NY * NZ) + py * NZ + pz, lax.div(px, 2) * 2 + pc)

    def x_shift(d):
        return lax.rem(x + d + NX, NX)

    def ring_device(axis, d):
        q = lax.rem(me[axis] + d + SIZE[axis], SIZE[axis])
        return device(x, q, z, core) if axis == "y" else device(x, y, q, core)

    right, left = device(x_shift(1), y, z, core), device(x_shift(-1), y, z, core)
    sibling = device(x, y, z, 1 - core)
    pair = (lax.rem(b + NY * NZ, 2 * NY * NZ), m)

    mine = pl.ds(pl.multiple_of(x_lo * ROWS, ROWS), ROWS)
    load_x = pltpu.make_async_copy(tok, gath.at[m, 0, mine, :], loc_sem.at[0])
    load_y = pltpu.make_async_copy(gout, gath.at[m, 1, mine, :], loc_sem.at[1])
    smalls = [
        pltpu.make_async_copy(source, dest, loc_sem.at[3 + i])
        for i, (source, dest) in enumerate(((code, code_s), (decode, decode_s), (strag, strag_s)))
    ]
    for load in (load_x, load_y, *smalls):
        load.start()

    barrier = pltpu.get_barrier_semaphore()
    partners = [right, left, sibling]
    partners += [ring_device(axis, d) for axis in ("y", "z") for d in (1, -1)]
    partners += [ring_device(axis, d) for axis in ("z",) for d in (2, -2)]
    for partner in partners:
        pl.semaphore_signal(barrier, inc=1, device_id=partner, device_id_type=MESH)

    for i, source in enumerate((w_gate, w_lin, w_out)):
        pltpu.make_async_copy(source, wts.at[i], loc_sem.at[2]).start()

    for load in smalls:
        load.wait()
    alive = (strag_s[0] != b) & (strag_s[1] != b) & (strag_s[2] != b) & (strag_s[3] != b)
    own_decode = jnp.where(alive, decode_s[0], 0.0)
    row_id = lax.broadcasted_iota(jnp.int32, (8, LANES), 0)
    coeffs = jnp.zeros((8, LANES), F32)
    for j in range(5):
        coeffs = jnp.where(row_id == j, own_decode * code_s[0, j], coeffs)
    tab[0, x_lo] = coeffs
    pl.semaphore_wait(barrier, len(partners))

    def remote(src, dst, ss, rs, to):
        return pltpu.make_async_remote_copy(
            src_ref=src, dst_ref=dst, send_sem=ss, recv_sem=rs, device_id=to, device_id_type=MESH
        )

    pending = []

    def go(src, dst, ss, rs, to, kept=pending):
        copy = remote(src, dst, ss, rs, to)
        copy.start()
        kept.append(copy)
        return copy

    shared = []

    def slot(px, pc, kind):
        rows = pl.ds(pl.multiple_of(lax.rem(px, 2) * ROWS, ROWS), ROWS)
        return gath.at[lax.div(px, 2) * 2 + pc, kind, rows, :]

    own_slot = [slot(x, core, k) for k in (0, 1)]
    swap = go(tab.at[0, x_lo], tab.at[0, x_lo], ws_sem.at[0], wr_sem.at[0], pair)
    load_x.wait()
    from_left = [None, None]
    from_right = [None, None]
    from_left[0] = go(own_slot[0], own_slot[0], gs_sem.at[0], gr_sem.at[0], right, shared)
    load_y.wait()
    from_right[1] = go(own_slot[1], own_slot[1], gs_sem.at[0], gr_sem.at[3], left, shared)
    from_left[1] = go(own_slot[1], own_slot[1], gs_sem.at[0], gr_sem.at[1], right, shared)
    from_right[0] = go(own_slot[0], own_slot[0], gs_sem.at[0], gr_sem.at[2], left, shared)
    sib = {}

    def to_sibling(rel, kind):
        src = slot(x_shift(rel), core, kind)
        idx = (rel % 4) * 2 + kind
        sib[rel, kind] = go(src, src, gs_sem.at[0], dr_sem.at[idx], sibling, shared)

    to_sibling(0, 0)
    to_sibling(0, 1)
    swap.wait_recv()
    near = [go(tab.at[0], tab.at[d], ws_sem.at[d], wr_sem.at[d], ring_device("z", d)) for d in (1, 2)]
    from_left[0].wait_recv()
    left_x = slot(x_shift(-1), core, 0)
    far_x = go(left_x, left_x, gs_sem.at[1], gr_sem.at[4], right, shared)
    to_sibling(-1, 0)
    from_right[1].wait_recv()
    right_y = slot(x_shift(1), core, 1)
    far_y = go(right_y, right_y, gs_sem.at[1], gr_sem.at[5], left, shared)
    to_sibling(1, 1)
    for copy in near:
        copy.wait_recv()
    farther = go(tab.at[pl.ds(1, 2)], tab.at[pl.ds(3, 2)], ws_sem.at[3], wr_sem.at[3], ring_device("z", 2))
    pltpu.make_async_copy(wts, wts, loc_sem.at[2]).wait()
    from_left[1].wait_recv()
    to_sibling(-1, 1)
    from_right[0].wait_recv()
    to_sibling(1, 0)

    def forward(mm, first, lower=0, upper=HID):
        ks = pl.ds(pl.multiple_of(mm * WIDTH, WIDTH), WIDTH)
        cols = slice(lower, upper)
        for i, (kind, acc) in enumerate(((0, acc_g), (0, acc_l), (1, acc_h))):
            part = jnp.dot(gath[mm, kind], wts[i, ks, cols], preferred_element_type=F32)
            acc[:, cols] = part if first else acc[:, cols] + part

    def transpose(a):
        tokens = pl.ds(pl.multiple_of(a * ROWS, ROWS), ROWS)
        for i in range(2):
            xt[pl.ds(i * WIDTH, WIDTH), tokens] = gath[2 * x_lo + i, 0, tokens, :].T
            yt[pl.ds(i * WIDTH, WIDTH), tokens] = gath[2 * x_lo + i, 1, tokens, :].T

    forward(2 * x_hi + core, True)
    for rel in (0, -1, 1):
        for kind in (0, 1):
            sib[rel, kind].wait_recv()
    farther.wait_recv()
    from_y = go(tab.at[pl.ds(1, 4)], ytab, ws_sem.at[4], wr_sem.at[4], ring_device("y", 1))
    forward(2 * x_hi + 1 - core, False)
    far_x.wait_recv()
    to_sibling(2, 0)
    far_y.wait_recv()
    to_sibling(2, 1)
    forward(2 * (1 - x_hi) + core, False)
    transpose(1 - x_lo)
    sib[2, 0].wait_recv()
    sib[2, 1].wait_recv()
    transpose(x_lo)
    from_y.wait_recv()
    weight = []
    for a in (0, 1):
        total = tab[0, a, 0:1, :]
        other = jnp.where(y == 0, 1 - a, a)
        for j in (1, 2, 3, 4):
            total = total + jnp.where(z >= j, tab[j, a, j : j + 1, :], ytab[j - 1, other, j : j + 1, :])
        weight.append(jnp.concatenate([total, total], axis=1))

    finished = set()

    def finish(block):
        lower, upper = BLOCKS[block]
        forward(2 * (1 - x_hi) + 1 - core, False, lower, upper)

        def elementwise(i, carry):
            rows = pl.ds(pl.multiple_of(i * 32, 32), 32)
            act, slope = gelu_parts(acc_g[rows, lower:upper])
            lin, dh = acc_l[rows, lower:upper], acc_h[rows, lower:upper]
            dmat[rows, lower:upper] = (dh * lin * slope).astype(BF16)
            dmat[rows, HID + lower : HID + upper] = (dh * act).astype(BF16)
            dmat[rows, 2 * HID + lower : 2 * HID + upper] = (act * lin).astype(BF16)
            return carry

        lax.fori_loop(0, 2 * ROWS // 32, elementwise, 0)

    def products(s):
        col, width = STREAMS[s][2:4]
        for block, (lower, upper) in enumerate(BLOCKS):
            if block not in finished and col % HID < upper and col % HID + width > lower:
                finished.add(block)
                finish(block)
        lhs = xt if col < 2 * HID else yt
        for yd in range(NY):
            rows = slice(yd * NZ * OWN, (yd + 1) * NZ * OWN)
            value = None
            for i in (0, 1):
                tokens = slice(i * ROWS, (i + 1) * ROWS)
                part = jnp.dot(lhs[rows, tokens], dmat[tokens, col : col + width], preferred_element_type=F32)
                part = weight[i][:, :width] * part
                value = part if value is None else value + part
            prod[yd, :, :, col : col + width] = value.reshape(NZ, OWN, width)

    def local1(s, d):
        axis, _, col, width = STREAMS[s][:4]
        cols = slice(col, col + width)
        return prod[:, d, :, cols] if axis == "z" else prod[d, :, :, cols]

    def run(s):
        axis1, axis2, col, width, sigma, two_stage = STREAMS[s]
        yield
        products(s)
        for phase, axis, snd, rcv in ((0, axis1, snd1[s], rcv1[s]), (1, axis2, snd2[s], rcv2[s])):
            n = SIZE[axis]
            local = functools.partial(local1, s) if phase == 0 else lambda d: mid[s][d]
            ss, base = s_sem.at[2 * s + phase], first_sem[s][phase]
            sent.append((snd, ss))
            messages, finals = schedule(n, sigma, phase and two_stage)
            middle = n - 1 - finals
            for direction, hops, distance, index, before in messages:
                yield
                value = local(lax.rem(me[axis] + direction * distance + n, n))
                to = ring_device(axis, direction * hops)
                if before is not None:
                    remote(snd.at[before], rcv.at[before], ss, r_sem.at[base + before], to).wait_recv()
                    value = value + rcv[before].astype(F32)
                snd[index] = value.astype(BF16)
                remote(snd.at[index], rcv.at[index], ss, r_sem.at[base + min(index, middle)], to).start()
            yield
            last = pl.ds(middle, finals)
            remote(snd.at[last], rcv.at[last], ss, r_sem.at[base + middle], sibling).wait_recv()
            arrived = range(middle, n - 1)
            value = local(me[axis])
            for index in arrived:
                value = value + rcv[index].astype(F32)
            if phase == 0:
                mid[s][...] = value
            else:
                kind, cols = col // HID, pl.ds(col % HID, width)
                out[kind, :, cols] = value

    first_sem, _ = counts()
    sent = []
    runs = [run(s) for s in range(n_streams)]
    for r in runs:
        next(r)
    for s in ORDER:
        next(runs[s], None)
    for snd, ss in sent:
        remote(snd, snd, ss, r_sem.at[0], sibling).wait_send()
    for copy in pending:
        copy.wait_send()
    assert len(shared) == 14
    remote(gath.at[0:3], gath.at[0:3], gs_sem.at[0], gr_sem.at[0], sibling).wait_send()
    remote(gath.at[3, 0], gath.at[3, 0], gs_sem.at[1], gr_sem.at[0], sibling).wait_send()


def shards(tokens, grad_out, w_gate, w_lin, w_out_t, code, decode, stragglers):
    n = len(STREAMS)
    scratch = [
        pltpu.SMEM((1, 5), F32),
        pltpu.SMEM((1,), F32),
        pltpu.SMEM((4,), jnp.int32),
        pltpu.VMEM((4, 2, 2 * ROWS, WIDTH), BF16),
        pltpu.VMEM((3, 4 * WIDTH, HID), BF16),
        pltpu.VMEM((2 * ROWS, HID), F32),
        pltpu.VMEM((2 * ROWS, HID), F32),
        pltpu.VMEM((2 * ROWS, HID), F32),
        pltpu.VMEM((2 * ROWS, 3 * HID), BF16),
        pltpu.VMEM((2 * WIDTH, 2 * ROWS), BF16),
        pltpu.VMEM((2 * WIDTH, 2 * ROWS), BF16),
        pltpu.VMEM((NY, NZ, OWN, 3 * HID), F32),
        pltpu.VMEM((5, 2, 8, LANES), F32),
        pltpu.VMEM((4, 2, 8, LANES), F32),
    ]
    first = [pltpu.VMEM((SIZE[a] - 1, SIZE[c], OWN, w), BF16) for a, c, _, w, _, _ in STREAMS]
    second = [pltpu.VMEM((SIZE[c] - 1, OWN, w), BF16) for a, c, _, w, _, _ in STREAMS]
    scratch += first + first + second + second
    scratch += [pltpu.VMEM((SIZE[c], OWN, w), F32) for a, c, _, w, _, _ in STREAMS]
    dma = pltpu.SemaphoreType.DMA
    scratch += [dma((6,)), dma((2,)), dma((6,)), dma((8,)), dma((5,)), dma((5,))]
    scratch += [dma((2 * n,)), dma((counts()[1],))]
    hbm = pl.BlockSpec(memory_space=pl.ANY)
    result = pl.pallas_call(
        kernel,
        out_shape=pltpu.VMEM((3, OWN, HID), F32),
        in_specs=[hbm] * 8,
        out_specs=pl.BlockSpec(memory_space=pltpu.VMEM),
        scratch_shapes=scratch,
        compiler_params=pltpu.CompilerParams(
            collective_id=0, has_side_effects=True, vmem_limit_bytes=60 * 1024 * 1024
        ),
    )(tokens, grad_out, w_gate, w_lin, w_out_t, code, decode, stragglers)
    return jnp.swapaxes(result, 0, 1)


def solution(mesh):
    in_specs = (
        P("blk", "mp"),
        P("blk", "mp"),
        P(None, "mp"),
        P(None, "mp"),
        P(None, "mp"),
        P("blk", None),
        P("blk"),
        P(),
    )
    out_specs = P("blk", None, "mp")
    return jax.shard_map(shards, mesh=mesh, in_specs=in_specs, out_specs=out_specs, check_vma=False)
```

```python
import functools

import jax
import jax.numpy as jnp
from jax import lax
from jax.experimental import pallas as pl
from jax.experimental.pallas import tpu as pltpu
from jax.sharding import PartitionSpec as P

MESH = pl.DeviceIdType.MESH
BF16 = jnp.bfloat16
F32 = jnp.float32

NX, NY, NZ = 4, 4, 8
SIZE = {"y": NY, "z": NZ}
ROWS = 128
WIDTH = 512
HID = 640
OWN = 32
LANES = 128

STREAMS = (
    ("y", "z", 1792, 128, 1, 1),
    ("z", "y", 1536, 128, 1, 1),
    ("z", "y", 1280, 256, -1, 0),
    ("z", "y", 1664, 128, 1, 0),
    ("y", "z", 1024, 256, -1, 1),
    ("y", "z", 0, 384, 1, 1),
    ("z", "y", 896, 128, 1, 1),
    ("z", "y", 384, 256, -1, 1),
    ("y", "z", 640, 256, -1, 1),
)
ORDER = (
    7, 7, 7, 3, 3, 0, 0, 3, 0, 4, 4, 4, 1, 1, 1, 2, 2, 2, 6, 6, 6, 5, 5, 8, 8, 5, 8, 7, 7, 0,
    3, 3, 1, 1, 2, 2, 4, 6, 6, 7, 7, 3, 3, 8, 1, 1, 5, 2, 2, 6, 6, 7, 3, 0, 0, 0, 0, 0, 1, 4,
    4, 4, 4, 4, 2, 6, 3, 3, 3, 7, 7, 7, 7, 5, 5, 8, 8, 8, 8, 5, 5, 8, 5, 0, 0, 1, 1, 1, 0, 1,
    4, 3, 4, 4, 6, 6, 6, 6, 2, 2, 2, 7, 5, 1, 8, 3, 8, 8, 5, 5, 2, 6, 0, 4, 8, 2, 5,
)
BLOCKS = ((0, 128), (128, 384), (384, 640))


def schedule(n, sigma, two_stage):
    half = n // 2
    if two_stage and n == 4:
        return [(sigma, 2, 2, 0, None), (1, 1, 1, 1, None), (-1, 1, 1, 2, None)], 3
    if two_stage:
        messages = [
            (sigma, 2, 4, 0, None),
            (sigma, 2, 3, 1, None),
            (-sigma, 2, 3, 2, None),
            (-sigma, 2, 2, 3, None),
            (sigma, 2, 2, 4, 0),
            (sigma, 1, 1, 5, 1),
            (-sigma, 1, 1, 6, 2),
        ]
        return messages, 4
    messages = []
    for t in range(1, half + 1):
        index = t - 1 if t < half else n - 3
        messages.append((sigma, 1, half + 1 - t, index, t - 2 if t > 1 else None))
        if t < half:
            index = half + t - 2 if t < half - 1 else n - 2
            messages.append((-sigma, 1, half - t, index, half + t - 3 if t > 1 else None))
    return messages, 2


def counts():
    first, total = [], 0
    for a, c, _, _, sigma, two_stage in STREAMS:
        middle = total + SIZE[a] - schedule(SIZE[a], sigma, 0)[1]
        first.append((total, middle))
        total = middle + SIZE[c] - schedule(SIZE[c], sigma, two_stage)[1]
    return first, total


def gelu_parts(u):
    c = 0.7978845608028654
    t = jnp.tanh(c * (u + 0.044715 * (u * u * u)))
    half = 0.5 * (1.0 + t)
    act = u * half
    slope = half + 0.5 * u * (1.0 - t * t) * (c * (1.0 + 3.0 * 0.044715 * (u * u)))
    return act, slope


def kernel(
    tok, gout, w_gate, w_lin, w_out, code, decode, strag,
    out,
    code_s, decode_s, strag_s,
    gath, wts, acc_g, acc_l, acc_h, dmat, xt, yt, prod, tab, ytab, *rest,
):
    n_streams = len(STREAMS)
    snd1, rcv1 = rest[:n_streams], rest[n_streams : 2 * n_streams]
    snd2, rcv2 = rest[2 * n_streams : 3 * n_streams], rest[3 * n_streams : 4 * n_streams]
    mid = rest[4 * n_streams : 5 * n_streams]
    (loc_sem, gs_sem, gr_sem, dr_sem, ws_sem, wr_sem, s_sem, r_sem) = rest[5 * n_streams :]

    b = lax.axis_index("blk")
    m = lax.axis_index("mp")
    x_lo, yz = lax.div(b, NY * NZ), lax.rem(b, NY * NZ)
    y, z = lax.div(yz, NZ), lax.rem(yz, NZ)
    x_hi, core = lax.div(m, 2), lax.rem(m, 2)
    x = 2 * x_hi + x_lo
    me = {"y": y, "z": z}

    def device(px, py, pz, pc):
        return (lax.rem(px, 2) * (NY * NZ) + py * NZ + pz, lax.div(px, 2) * 2 + pc)

    def x_shift(d):
        return lax.rem(x + d + NX, NX)

    def ring_device(axis, d):
        q = lax.rem(me[axis] + d + SIZE[axis], SIZE[axis])
        return device(x, q, z, core) if axis == "y" else device(x, y, q, core)

    right, left = device(x_shift(1), y, z, core), device(x_shift(-1), y, z, core)
    sibling = device(x, y, z, 1 - core)
    pair = (lax.rem(b + NY * NZ, 2 * NY * NZ), m)

    mine = pl.ds(pl.multiple_of(x_lo * ROWS, ROWS), ROWS)
    load_x = pltpu.make_async_copy(tok, gath.at[m, 0, mine, :], loc_sem.at[0])
    load_y = pltpu.make_async_copy(gout, gath.at[m, 1, mine, :], loc_sem.at[1])
    smalls = [
        pltpu.make_async_copy(source, dest, loc_sem.at[3 + i])
        for i, (source, dest) in enumerate(((code, code_s), (decode, decode_s), (strag, strag_s)))
    ]
    for load in (load_x, load_y, *smalls):
        load.start()

    barrier = pltpu.get_barrier_semaphore()
    partners = [right, left, sibling]
    partners += [ring_device(axis, d) for axis in ("y", "z") for d in (1, -1)]
    partners += [ring_device(axis, d) for axis in ("y", "z",) for d in (2, -2)]
    for partner in partners:
        pl.semaphore_signal(barrier, inc=1, device_id=partner, device_id_type=MESH)

    for i, source in enumerate((w_gate, w_lin, w_out)):
        pltpu.make_async_copy(source, wts.at[i], loc_sem.at[2]).start()

    for load in smalls:
        load.wait()
    alive = (strag_s[0] != b) & (strag_s[1] != b) & (strag_s[2] != b) & (strag_s[3] != b)
    own_decode = jnp.where(alive, decode_s[0], 0.0)
    row_id = lax.broadcasted_iota(jnp.int32, (8, LANES), 0)
    coeffs = jnp.zeros((8, LANES), F32)
    for j in range(5):
        coeffs = jnp.where(row_id == j, own_decode * code_s[0, j], coeffs)
    tab[0, x_lo] = coeffs
    pl.semaphore_wait(barrier, len(partners))

    def remote(src, dst, ss, rs, to):
        return pltpu.make_async_remote_copy(
            src_ref=src, dst_ref=dst, send_sem=ss, recv_sem=rs, device_id=to, device_id_type=MESH
        )

    pending = []

    def go(src, dst, ss, rs, to, kept=pending):
        copy = remote(src, dst, ss, rs, to)
        copy.start()
        kept.append(copy)
        return copy

    shared = []

    def slot(px, pc, kind):
        rows = pl.ds(pl.multiple_of(lax.rem(px, 2) * ROWS, ROWS), ROWS)
        return gath.at[lax.div(px, 2) * 2 + pc, kind, rows, :]

    own_slot = [slot(x, core, k) for k in (0, 1)]
    swap = go(tab.at[0, x_lo], tab.at[0, x_lo], ws_sem.at[0], wr_sem.at[0], pair)
    load_x.wait()
    from_left = [None, None]
    from_right = [None, None]
    from_left[0] = go(own_slot[0], own_slot[0], gs_sem.at[0], gr_sem.at[0], right, shared)
    load_y.wait()
    from_right[1] = go(own_slot[1], own_slot[1], gs_sem.at[0], gr_sem.at[3], left, shared)
    from_left[1] = go(own_slot[1], own_slot[1], gs_sem.at[0], gr_sem.at[1], right, shared)
    from_right[0] = go(own_slot[0], own_slot[0], gs_sem.at[0], gr_sem.at[2], left, shared)
    sib = {}

    def to_sibling(rel, kind):
        src = slot(x_shift(rel), core, kind)
        idx = (rel % 4) * 2 + kind
        sib[rel, kind] = go(src, src, gs_sem.at[0], dr_sem.at[idx], sibling, shared)

    to_sibling(0, 0)
    to_sibling(0, 1)
    swap.wait_recv()
    near = [go(tab.at[0], tab.at[d], ws_sem.at[d], wr_sem.at[d], ring_device("z", d)) for d in (1, 2)]
    from_left[0].wait_recv()
    left_x = slot(x_shift(-1), core, 0)
    far_x = go(left_x, left_x, gs_sem.at[1], gr_sem.at[4], right, shared)
    to_sibling(-1, 0)
    from_right[1].wait_recv()
    right_y = slot(x_shift(1), core, 1)
    far_y = go(right_y, right_y, gs_sem.at[1], gr_sem.at[5], left, shared)
    to_sibling(1, 1)
    for copy in near:
        copy.wait_recv()
    farther = go(tab.at[pl.ds(1, 2)], tab.at[pl.ds(3, 2)], ws_sem.at[3], wr_sem.at[3], ring_device("z", 2))
    pltpu.make_async_copy(wts, wts, loc_sem.at[2]).wait()
    from_left[1].wait_recv()
    to_sibling(-1, 1)
    from_right[0].wait_recv()
    to_sibling(1, 0)

    def forward(mm, first, lower=0, upper=HID):
        ks = pl.ds(pl.multiple_of(mm * WIDTH, WIDTH), WIDTH)
        cols = slice(lower, upper)
        for i, (kind, acc) in enumerate(((0, acc_g), (0, acc_l), (1, acc_h))):
            part = jnp.dot(gath[mm, kind], wts[i, ks, cols], preferred_element_type=F32)
            acc[:, cols] = part if first else acc[:, cols] + part

    def transpose(a):
        tokens = pl.ds(pl.multiple_of(a * ROWS, ROWS), ROWS)
        for i in range(2):
            xt[pl.ds(i * WIDTH, WIDTH), tokens] = gath[2 * x_lo + i, 0, tokens, :].T
            yt[pl.ds(i * WIDTH, WIDTH), tokens] = gath[2 * x_lo + i, 1, tokens, :].T

    forward(2 * x_hi + core, True)
    for rel in (0, -1, 1):
        for kind in (0, 1):
            sib[rel, kind].wait_recv()
    farther.wait_recv()
    from_y = go(tab.at[pl.ds(1, 4)], ytab, ws_sem.at[4], wr_sem.at[4], ring_device("y", 1))
    forward(2 * x_hi + 1 - core, False)
    far_x.wait_recv()
    to_sibling(2, 0)
    far_y.wait_recv()
    to_sibling(2, 1)
    forward(2 * (1 - x_hi) + core, False)
    transpose(1 - x_lo)
    sib[2, 0].wait_recv()
    sib[2, 1].wait_recv()
    transpose(x_lo)
    from_y.wait_recv()
    weight = []
    for a in (0, 1):
        total = tab[0, a, 0:1, :]
        other = jnp.where(y == 0, 1 - a, a)
        for j in (1, 2, 3, 4):
            total = total + jnp.where(z >= j, tab[j, a, j : j + 1, :], ytab[j - 1, other, j : j + 1, :])
        weight.append(jnp.concatenate([total] * 4, axis=1))

    finished = set()

    def finish(block):
        lower, upper = BLOCKS[block]
        chunk = 16384 // (upper - lower)
        forward(2 * (1 - x_hi) + 1 - core, False, lower, upper)

        def elementwise(i, carry):
            rows = pl.ds(pl.multiple_of(i * chunk, chunk), chunk)
            act, slope = gelu_parts(acc_g[rows, lower:upper])
            lin, dh = acc_l[rows, lower:upper], acc_h[rows, lower:upper]
            dmat[rows, lower:upper] = (dh * lin * slope).astype(BF16)
            dmat[rows, HID + lower : HID + upper] = (dh * act).astype(BF16)
            dmat[rows, 2 * HID + lower : 2 * HID + upper] = (act * lin).astype(BF16)
            return carry

        lax.fori_loop(0, 2 * ROWS // chunk, elementwise, 0)

    def products(s):
        col, width = STREAMS[s][2:4]
        for block, (lower, upper) in enumerate(BLOCKS):
            if block not in finished and col % HID < upper and col % HID + width > lower:
                finished.add(block)
                finish(block)
        lhs = xt if col < 2 * HID else yt
        for yd in range(NY):
            rows = slice(yd * NZ * OWN, (yd + 1) * NZ * OWN)
            value = None
            for i in (0, 1):
                tokens = slice(i * ROWS, (i + 1) * ROWS)
                part = jnp.dot(lhs[rows, tokens], dmat[tokens, col : col + width], preferred_element_type=F32)
                part = weight[i][:, :width] * part
                value = part if value is None else value + part
            prod[yd, :, :, col : col + width] = value.reshape(NZ, OWN, width)

    def local1(s, d):
        axis, _, col, width = STREAMS[s][:4]
        cols = slice(col, col + width)
        return prod[:, d, :, cols] if axis == "z" else prod[d, :, :, cols]

    def run(s):
        axis1, axis2, col, width, sigma, two_stage = STREAMS[s]
        yield
        products(s)
        for phase, axis, snd, rcv in ((0, axis1, snd1[s], rcv1[s]), (1, axis2, snd2[s], rcv2[s])):
            n = SIZE[axis]
            local = functools.partial(local1, s) if phase == 0 else lambda d: mid[s][d]
            ss, base = s_sem.at[2 * s + phase], first_sem[s][phase]
            sent.append((snd, ss))
            messages, finals = schedule(n, sigma, phase and two_stage)
            middle = n - 1 - finals
            for direction, hops, distance, index, before in messages:
                yield
                value = local(lax.rem(me[axis] + direction * distance + n, n))
                to = ring_device(axis, direction * hops)
                if before is not None:
                    remote(snd.at[before], rcv.at[before], ss, r_sem.at[base + before], to).wait_recv()
                    value = value + rcv[before].astype(F32)
                snd[index] = value.astype(BF16)
                remote(snd.at[index], rcv.at[index], ss, r_sem.at[base + min(index, middle)], to).start()
            yield
            last = pl.ds(middle, finals)
            remote(snd.at[last], rcv.at[last], ss, r_sem.at[base + middle], sibling).wait_recv()
            arrived = range(middle, n - 1)
            value = local(me[axis])
            for index in arrived:
                value = value + rcv[index].astype(F32)
            if phase == 0:
                mid[s][...] = value
            else:
                kind, cols = col // HID, pl.ds(col % HID, width)
                out[kind, :, cols] = value

    first_sem, _ = counts()
    sent = []
    runs = [run(s) for s in range(n_streams)]
    for r in runs:
        next(r)
    for s in ORDER:
        next(runs[s], None)
    for snd, ss in sent:
        remote(snd, snd, ss, r_sem.at[0], sibling).wait_send()
    for copy in pending:
        copy.wait_send()
    assert len(shared) == 14
    remote(gath.at[0:3], gath.at[0:3], gs_sem.at[0], gr_sem.at[0], sibling).wait_send()
    remote(gath.at[3, 0], gath.at[3, 0], gs_sem.at[1], gr_sem.at[0], sibling).wait_send()


def shards(tokens, grad_out, w_gate, w_lin, w_out_t, code, decode, stragglers):
    n = len(STREAMS)
    scratch = [
        pltpu.SMEM((1, 5), F32),
        pltpu.SMEM((1,), F32),
        pltpu.SMEM((4,), jnp.int32),
        pltpu.VMEM((4, 2, 2 * ROWS, WIDTH), BF16),
        pltpu.VMEM((3, 4 * WIDTH, HID), BF16),
        pltpu.VMEM((2 * ROWS, HID), F32),
        pltpu.VMEM((2 * ROWS, HID), F32),
        pltpu.VMEM((2 * ROWS, HID), F32),
        pltpu.VMEM((2 * ROWS, 3 * HID), BF16),
        pltpu.VMEM((2 * WIDTH, 2 * ROWS), BF16),
        pltpu.VMEM((2 * WIDTH, 2 * ROWS), BF16),
        pltpu.VMEM((NY, NZ, OWN, 3 * HID), F32),
        pltpu.VMEM((5, 2, 8, LANES), F32),
        pltpu.VMEM((4, 2, 8, LANES), F32),
    ]
    first = [pltpu.VMEM((SIZE[a] - 1, SIZE[c], OWN, w), BF16) for a, c, _, w, _, _ in STREAMS]
    second = [pltpu.VMEM((SIZE[c] - 1, OWN, w), BF16) for a, c, _, w, _, _ in STREAMS]
    scratch += first + first + second + second
    scratch += [pltpu.VMEM((SIZE[c], OWN, w), F32) for a, c, _, w, _, _ in STREAMS]
    dma = pltpu.SemaphoreType.DMA
    scratch += [dma((6,)), dma((2,)), dma((6,)), dma((8,)), dma((5,)), dma((5,))]
    scratch += [dma((2 * n,)), dma((counts()[1],))]
    hbm = pl.BlockSpec(memory_space=pl.ANY)
    result = pl.pallas_call(
        kernel,
        out_shape=pltpu.VMEM((3, OWN, HID), F32),
        in_specs=[hbm] * 8,
        out_specs=pl.BlockSpec(memory_space=pltpu.VMEM),
        scratch_shapes=scratch,
        compiler_params=pltpu.CompilerParams(
            collective_id=0, has_side_effects=True, vmem_limit_bytes=60 * 1024 * 1024
        ),
    )(tokens, grad_out, w_gate, w_lin, w_out_t, code, decode, stragglers)
    return jnp.swapaxes(result, 0, 1)


def solution(mesh):
    in_specs = (
        P("blk", "mp"),
        P("blk", "mp"),
        P(None, "mp"),
        P(None, "mp"),
        P(None, "mp"),
        P("blk", None),
        P("blk"),
        P(),
    )
    out_specs = P("blk", None, "mp")
    return jax.shard_map(shards, mesh=mesh, in_specs=in_specs, out_specs=out_specs, check_vma=False)
```
